32 devices in a mesh: sta: 8 (over z, y), seg: 4 (over x, core).
Axes of the slice: x: 2, y: 2, z: 4, core: 2. Of those that a mesh axis runs over, the one named last changes fastest.
Arguments:
- spectra: bfloat16 [2, 8, 512, 4096], P(None, 'seg', None, 'sta'), may hold values from -6 to 6
- bin_index: int32 [512], replicated, may hold values from 0 to 4096
Outputs:
- correlation: float32 [2, 4096, 4096], P(None, ('sta', 'seg'))
The draws below stay inside these ranges and needn't reach their ends.
All inputs are finite; a program needn't handle non-finite values.
Results may differ from the reference program's by a relative error of at most 0.012.
Values may be sent and summed in bfloat16 or wider, within the bound.
A program may use at most 64 MiB of HBM per device.

```python
import math
import jax
import jax.numpy as jnp
from jax import lax

S = 4096
NFFT = 8192
F = 512
SEG_DEV = 2
LAGS = 2
LAG_STEP = 37
HALF = 64
SEGMENTS = 8
N_SEG = 4


def with_ends(array, own_key, low, top_value):
    shape = array.shape
    index_at = [jax.random.randint(jax.random.fold_in(own_key, axis), (), 0, shape[axis]) for axis in range(len(shape))]
    array = array.at[tuple(index_at)].set(low)
    longest = shape.index(max(shape))
    index_at[longest] = (index_at[longest] + 1) % shape[longest]
    return array.at[tuple(index_at)].set(top_value)


def level_of(key, extent, pieces, least, high):
    def one(position, parts):
        draws = jax.random.uniform(jax.random.fold_in(jax.random.fold_in(key, 6), position), (parts,), jnp.float32, least / len(pieces), high / len(pieces))
        return jnp.repeat(jnp.exp(draws), extent[position] // parts).reshape((-1,) + (1,) * (len(extent) - position - 1))

    loudness = one(*pieces[0])
    for cut in pieces[1:]:
        loudness = loudness * one(*cut)
    return loudness


def gaussian(rng, dims, width, limit, pieces=(), kind=jnp.bfloat16):
    result = jax.random.normal(rng, dims, jnp.float32) * width
    if len(pieces) > 0:
        result = level_of(rng, dims, pieces, -0.22, 0.18) * result
    return jnp.clip(result, min=-limit, max=limit).astype(kind)


def setup_inputs(seed: int = 0) -> dict:
    keys = jax.random.split(jax.random.key(seed), 3)
    spectra = gaussian(keys[0], (2, SEGMENTS, F, S), 1.0, 6.0, ((1, 4), (3, 8)))
    bin_index = with_ends(jax.random.randint(keys[1], (F,), 0, NFFT // 2 + 1), jax.random.fold_in(keys[1], 1), 0, (NFFT // 2 + 1) - 1).astype(jnp.int32)
    return {"spectra": spectra, "bin_index": bin_index}


def whiten(spectra):
    values = spectra.astype(jnp.float32)
    energy = values[0] * values[0] + values[1] * values[1]
    freq_bins = values.shape[2]
    bin_pos = jnp.arange(freq_bins, dtype=jnp.int32)
    window = (jnp.abs(bin_pos[:, None] - bin_pos[None, :]) <= HALF).astype(jnp.float32)
    bin_count = lax.optimization_barrier(jnp.sum(window, axis=1))
    smoothed = jnp.einsum('gf,sfc->sgc', window, energy, precision=lax.Precision.HIGHEST) / bin_count[None, :, None]
    return (values / jnp.sqrt(smoothed + 1e-06)[None]).astype(jnp.bfloat16)

def phases(bin_index):
    lag_samples = (jnp.arange(LAGS, dtype=jnp.int32) + 1) * LAG_STEP
    phase_turn = lag_samples[:, None] * bin_index[None, :].astype(jnp.int32) % NFFT
    phase_angle = 2.0 * math.pi / NFFT * phase_turn.astype(jnp.float32)
    return (jnp.cos(phase_angle), jnp.sin(phase_angle))

def rotate(whitened, cosine, sine_part):
    real_part = whitened[0].astype(jnp.float32)[None]
    imag_part = whitened[1].astype(jnp.float32)[None]
    cos_part = cosine[:, None, :, None]
    sin_part = sine_part[:, None, :, None]
    rot_real = real_part * cos_part - imag_part * sin_part
    rot_imag = real_part * sin_part + imag_part * cos_part
    stacked = jnp.stack([rot_real, rot_imag], axis=1).astype(jnp.bfloat16)
    return stacked.reshape(cosine.shape[0], -1, whitened.shape[3])

def reference(spectra, bin_index):
    whitened = whiten(spectra)
    cosine, sine_part = phases(bin_index)
    norm_scale = 1.0 / math.sqrt(SEGMENTS * F)
    stations = whitened.shape[3]

    def add_group(group_idx, total):
        first_seg = (group_idx * SEG_DEV).astype(jnp.int32)
        group_spec = lax.dynamic_slice_in_dim(whitened, first_seg, SEG_DEV, 1)
        rotated = rotate(group_spec, cosine, sine_part).astype(jnp.float32)
        columns = group_spec.reshape(-1, stations).astype(jnp.float32)
        product = jnp.einsum('mki,kj->mij', rotated, columns, precision=lax.Precision.HIGHEST)
        stacked = lax.optimization_barrier((product * norm_scale).astype(jnp.bfloat16))
        return total + stacked.astype(jnp.float32)
    zero_total = jnp.zeros((LAGS, stations, stations), jnp.float32)
    return lax.fori_loop(0, N_SEG, add_group, zero_total)
```

```python
import functools
import math

import jax
import jax.numpy as jnp
from jax import lax
from jax.experimental import pallas as pl
from jax.experimental.pallas import tpu as pltpu
from jax.sharding import PartitionSpec as P

NFFT = 8192
LAGS = 2
LAG_STEP = 37
HALF = 64
MESH = pl.DeviceIdType.MESH


def whiten(spectra):
    values = spectra.astype(jnp.float32)
    energy = values[0] * values[0] + values[1] * values[1]
    freq_bins = values.shape[2]
    bin_pos = jnp.arange(freq_bins, dtype=jnp.int32)
    window = (jnp.abs(bin_pos[:, None] - bin_pos[None, :]) <= HALF).astype(jnp.float32)
    bin_count = jnp.sum(window, axis=1)
    smoothed = (
        jnp.einsum("gf,sfc->sgc", window, energy, precision=lax.Precision.HIGHEST)
        / bin_count[None, :, None]
    )
    return (values / jnp.sqrt(smoothed + 1e-06)[None]).astype(jnp.bfloat16)


def phases(bin_index):
    lag_samples = (jnp.arange(LAGS, dtype=jnp.int32) + 1) * LAG_STEP
    phase_turn = lag_samples[:, None] * bin_index[None, :] % NFFT
    phase_angle = 2.0 * math.pi / NFFT * phase_turn.astype(jnp.float32)
    return (jnp.cos(phase_angle), jnp.sin(phase_angle))


def rotate(whitened, cosine, sine_part):
    real_part = whitened[0].astype(jnp.float32)[None]
    imag_part = whitened[1].astype(jnp.float32)[None]
    cos_part = cosine[:, None, :, None]
    sin_part = sine_part[:, None, :, None]
    rot_real = real_part * cos_part - imag_part * sin_part
    rot_imag = real_part * sin_part + imag_part * cos_part
    stacked = jnp.stack([rot_real, rot_imag], axis=1).astype(jnp.bfloat16)
    return stacked.reshape(cosine.shape[0], -1, whitened.shape[3])


def pair_block(rotated, columns, norm_scale):
    product = jnp.einsum("mki,kj->mij", rotated, columns, preferred_element_type=jnp.float32)
    return (product * norm_scale).astype(jnp.bfloat16)


def general_body(spectra, bin_index):
    whitened = whiten(spectra)
    cosine, sine_part = phases(bin_index)
    seg_local = whitened.shape[1]
    freq_bins = whitened.shape[2]
    norm_scale = 1.0 / math.sqrt(seg_local * lax.axis_size("seg") * freq_bins)
    rotated = rotate(whitened, cosine, sine_part)
    shard_cols = lax.all_gather(whitened, "sta", axis=3, tiled=True)
    columns = shard_cols.reshape(-1, shard_cols.shape[3])
    product = pair_block(rotated, columns, norm_scale)
    return lax.psum_scatter(product, "seg", scatter_dimension=1, tiled=True).astype(jnp.float32)


OWN, SIDE, END, END_SIDE, MID, FAR = 0, 2, 4, 6, 8, 10


def kernel(
    dims, src, cos_ref, sin_ref, out, cols, raw_kept, rows, part, from_core, from_x, window, inv_count, split,
    load_sem, send_sem, recv_sem, core_send, core_recv, x_send, x_recv, out_send, out_recv,
):
    segs, bins, chunk, scale = dims
    depth = 2 * segs * bins
    half = segs * bins
    quarter = chunk // 2
    sta = lax.axis_index("sta")
    seg = lax.axis_index("seg")
    z, y = sta // 2, sta % 2
    x, core = seg // 2, seg % 2
    z_near = z + 1 - 2 * (z % 2)
    is_mid = ((z + 1) // 2) % 2
    side = z * 2 + (1 - y)
    near = z_near * 2 + y
    near_side = z_near * 2 + (1 - y)
    mid = (3 - z) * 2 + y
    far = ((z + 2) % 4) * 2 + y
    core_seg = x * 2 + (1 - core)
    x_seg = (1 - x) * 2 + core
    station_of = {OWN: sta, SIDE: side, END: near, END_SIDE: near_side, MID: mid, FAR: far}

    barrier = pltpu.get_barrier_semaphore()
    for partner in ((sta, core_seg), (sta, x_seg), (side, seg), (near, seg), (near_side, seg)):
        pl.semaphore_signal(barrier, inc=1, device_id=partner, device_id_type=MESH)

    @pl.when(is_mid == 1)
    def _():
        pl.semaphore_signal(barrier, inc=1, device_id=(mid, seg), device_id_type=MESH)

    loads = [
        pltpu.make_async_copy(
            src.at[:, pl.ds(ch * chunk, chunk)], cols.at[OWN + ch], load_sem.at[ch]
        )
        for ch in range(2)
    ]
    for load in loads:
        load.start()
    pl.semaphore_wait(barrier, 5 + is_mid)

    def remote(source, target, send, recv, to_sta, to_seg):
        return pltpu.make_async_remote_copy(
            src_ref=source, dst_ref=target, send_sem=send, recv_sem=recv,
            device_id=(to_sta, to_seg), device_id_type=MESH,
        )

    def own_chunk(ch):
        return src.at[:, pl.ds(ch * chunk, chunk)]

    def landing(slot, ends):
        kept = SIDE if ends else END
        return raw_kept.at[slot - kept] if kept <= slot < kept + 2 else cols.at[slot]

    def push(source, target, slot, index, to_sta):
        copy = remote(source, target, send_sem.at[index], recv_sem.at[slot], to_sta, seg)
        copy.start()
        return copy

    def arrived(slot, ends):
        there = landing(slot, ends)
        remote(there, there, send_sem.at[0], recv_sem.at[slot], side, seg).wait_recv()

    row_at = lax.broadcasted_iota(jnp.int32, (bins, bins), 0)
    col_at = lax.broadcasted_iota(jnp.int32, (bins, bins), 1)
    band = jnp.where(jnp.abs(row_at - col_at) <= HALF, 1.0, 0.0).astype(jnp.bfloat16)
    window[:, :bins] = band
    window[:, bins:] = band
    pos = lax.broadcasted_iota(jnp.int32, (bins, chunk), 0)
    count = jnp.minimum(pos, HALF) + jnp.minimum(bins - 1 - pos, HALF) + 1
    inv_count[...] = 1.0 / count.astype(jnp.float32)

    def whiten_chunk(slot, ends):
        raw = landing(slot, ends)

        def one(s, carry):
            at_re = pl.ds(pl.multiple_of(s * bins, bins), bins)
            at_im = pl.ds(pl.multiple_of(half + s * bins, bins), bins)
            real = raw[at_re, :].astype(jnp.float32)
            imag = raw[at_im, :].astype(jnp.float32)
            energy = real * real + imag * imag
            high = energy.astype(jnp.bfloat16)
            split[:bins, :] = high
            split[bins:, :] = (energy - high.astype(jnp.float32)).astype(jnp.bfloat16)
            total = jnp.dot(window[...], split[...], preferred_element_type=jnp.float32)
            gain = lax.rsqrt(total * inv_count[...] + 1e-06)
            real = raw[at_re, :].astype(jnp.float32)
            imag = raw[at_im, :].astype(jnp.float32)
            cols[slot, at_re, :] = (real * gain).astype(jnp.bfloat16)
            cols[slot, at_im, :] = (imag * gain).astype(jnp.bfloat16)
            return carry

        lax.fori_loop(0, segs, one, 0)

    def rotate_chunk(row, slot):
        xq = slot % 2

        def one(step, carry):
            parity, s = step // segs, step % segs
            lanes = pl.ds(pl.multiple_of(parity * quarter, quarter), quarter)
            at_re = pl.ds(pl.multiple_of(s * bins, bins), bins)
            at_im = pl.ds(pl.multiple_of(half + s * bins, bins), bins)
            real = cols[slot, at_re, lanes].T.astype(jnp.float32)
            imag = cols[slot, at_im, lanes].T.astype(jnp.float32)
            for lag in range(LAGS):
                cosine = cos_ref[lag : lag + 1, :]
                sine = sin_ref[lag : lag + 1, :]
                at = pl.ds(xq * LAGS * quarter + lag * quarter, quarter)
                rows[row, parity, at, at_re] = (real * cosine - imag * sine).astype(jnp.bfloat16)
                rows[row, parity, at, at_im] = (real * sine + imag * cosine).astype(jnp.bfloat16)
            return carry

        lax.fori_loop(0, 2 * segs, one, 0)

    def core_copy(task):
        return remote(part.at[task, 0], from_core.at[task], core_send.at[task], core_recv.at[task], sta, core_seg)

    def x_copy(task):
        return remote(part.at[task, 1, 1 - x], from_x.at[task], x_send.at[task], x_recv.at[task], sta, x_seg)

    def columns_at(slot):
        start = (station_of[slot - slot % 2] * 2 + slot % 2) * chunk
        return pl.ds(pl.multiple_of(start, chunk), chunk)

    def out_copy(task, row, slot):
        source = part.at[task, 1, x]
        target = out.at[:, columns_at(slot)]
        if row == 0:
            return pltpu.make_async_copy(source, target, out_send.at[task])
        index = slot - 4 if row == 3 else slot
        to_sta = {1: side, 2: near, 3: near_side}[row]
        return remote(source, target, out_send.at[task], out_recv.at[index], to_sta, seg)

    def compute(task, row, slot):
        def one(h, carry):
            parity = (core + 1 + h) % 2
            product = jnp.dot(rows[row, parity], cols[slot], preferred_element_type=jnp.float32)
            product = (product * scale).astype(jnp.bfloat16)
            part[task, h, 0] = product[: LAGS * quarter]
            part[task, h, 1] = product[LAGS * quarter :]
            return carry

        lax.fori_loop(0, 2, one, 0)
        core_copy(task).start()

    def add_into(target, other):
        target[...] = (target[...].astype(jnp.float32) + other[...].astype(jnp.float32)).astype(jnp.bfloat16)

    def finish_core(task, row, slot):
        core_copy(task).wait_recv()
        add_into(part.at[task, 1, 1 - x], from_core.at[task, 1 - x])
        x_copy(task).start()
        add_into(part.at[task, 1, x], from_core.at[task, x])

    def finish_x(task, row, slot):
        x_copy(task).wait_recv()
        add_into(part.at[task, 1, x], from_x.at[task])
        out_copy(task, row, slot).start()

    class Flow:
        def __init__(self):
            self.done = []
            self.at_core = 0
            self.at_x = 0

        def task(self, row, slot, core_lag=1, x_lag=3):
            compute(len(self.done), row, slot)
            self.done.append((len(self.done), row, slot))
            self.advance(core_lag, x_lag)

        def advance(self, core_lag, x_lag):
            while self.at_core < len(self.done) - core_lag:
                finish_core(*self.done[self.at_core])
                self.at_core += 1
            while self.at_x < len(self.done) - x_lag:
                finish_x(*self.done[self.at_x])
                self.at_x += 1

        def drain(self):
            self.advance(0, 0)
            for task in self.done:
                core_copy(task[0]).wait_send()
                x_copy(task[0]).wait_send()
                copy = out_copy(*task)
                copy.wait() if task[1] == 0 else copy.wait_send()

    def incoming(index):
        target = out.at[:, pl.ds(0, chunk)]
        remote(target, target, out_send.at[0], out_recv.at[index], side, seg).wait_recv()

    def start_own(flow, ends):
        for ch in range(2):
            loads[ch].wait()
            whiten_chunk(OWN + ch, ends)
            rotate_chunk(0, OWN + ch)
        for ch in range(2):
            flow.task(0, OWN + ch)

    def leave(flow, sends, expected):
        flow.drain()
        for copy in sends:
            copy.wait_send()
        for index in expected:
            incoming(index)

    @pl.when(is_mid == 0)
    def _():
        sends = []
        for ch in range(2):
            sends.append(push(own_chunk(ch), raw_kept.at[ch], SIDE + ch, ch, side))
            sends.append(push(own_chunk(ch), raw_kept.at[ch], END + ch, 2 + ch, near))
        flow = Flow()
        start_own(flow, True)
        for ch in range(2):
            arrived(SIDE + ch, True)
            if ch == 0:
                sends.append(push(raw_kept.at[0], cols.at[END_SIDE], END_SIDE, 4, near))
            whiten_chunk(SIDE + ch, True)
            flow.task(0, SIDE + ch)
        leave(flow, sends, (0, 1, 2, 3, 4, 5, 6, 7, 8, 9, 10, 11))

    @pl.when(is_mid == 1)
    def _():
        sends = []
        for ch in range(2):
            sends.append(push(own_chunk(ch), cols.at[SIDE + ch], SIDE + ch, ch, side))
            sends.append(push(own_chunk(ch), cols.at[MID + ch], MID + ch, 2 + ch, mid))

        def take(slot, row=None):
            arrived(slot, False)
            if END <= slot < END + 2:
                ch = slot - END
                sends.append(push(raw_kept.at[ch], cols.at[FAR + ch], FAR + ch, 4 + ch, mid))
                if ch == 1:
                    sends.append(push(raw_kept.at[1], cols.at[END_SIDE + 1], END_SIDE + 1, 6, side))
            whiten_chunk(slot, False)
            if row is not None:
                rotate_chunk(row, slot)

        flow = Flow()
        start_own(flow, False)
        take(END, 2)
        flow.task(0, END)
        take(SIDE, 1)
        flow.task(0, SIDE)
        take(MID)
        flow.task(0, MID)
        take(END + 1, 2)
        flow.task(0, END + 1)
        for slot in (OWN, OWN + 1, SIDE, MID):
            flow.task(2, slot)
        take(SIDE + 1, 1)
        flow.task(2, SIDE + 1)
        flow.task(0, SIDE + 1)
        flow.task(1, MID)
        take(MID + 1)
        for row in (2, 1, 0):
            flow.task(row, MID + 1)
        take(END_SIDE, 3)
        flow.task(0, END_SIDE)
        take(END_SIDE + 1, 3)
        flow.task(0, END_SIDE + 1)
        flow.task(3, MID)
        flow.task(3, MID + 1)
        for ch in range(2):
            take(FAR + ch)
            for row in (3, 2, 1, 0):
                flow.task(row, FAR + ch)
        leave(flow, sends, (8, 9, 10, 11))


def fused_body(spectra, bin_index):
    cosine, sine_part = phases(bin_index)
    parts, segs, bins, stations = spectra.shape
    blocks = lax.axis_size("sta")
    depth = parts * segs * bins
    chunk = stations // 2
    quarter = chunk // 2
    scale = 1.0 / math.sqrt(segs * lax.axis_size("seg") * bins)
    tasks = 28
    low = jnp.bfloat16
    out = pl.pallas_call(
        functools.partial(kernel, (segs, bins, chunk, scale)),
        out_shape=jax.ShapeDtypeStruct((LAGS * quarter, blocks * stations), low),
        in_specs=[
            pl.BlockSpec(memory_space=pl.ANY),
            pl.BlockSpec(memory_space=pltpu.VMEM),
            pl.BlockSpec(memory_space=pltpu.VMEM),
        ],
        out_specs=pl.BlockSpec(memory_space=pl.ANY),
        scratch_shapes=[
            pltpu.VMEM((12, depth, chunk), low),
            pltpu.VMEM((2, depth, chunk), low),
            pltpu.VMEM((4, 2, LAGS * chunk, depth), low),
            pltpu.VMEM((tasks, 2, 2, LAGS * quarter, chunk), low),
            pltpu.VMEM((tasks, 2, LAGS * quarter, chunk), low),
            pltpu.VMEM((tasks, LAGS * quarter, chunk), low),
            pltpu.VMEM((bins, 2 * bins), low),
            pltpu.VMEM((bins, chunk), jnp.float32),
            pltpu.VMEM((2 * bins, chunk), low),
            pltpu.SemaphoreType.DMA((2,)),
            pltpu.SemaphoreType.DMA((7,)),
            pltpu.SemaphoreType.DMA((12,)),
            pltpu.SemaphoreType.DMA((tasks,)),
            pltpu.SemaphoreType.DMA((tasks,)),
            pltpu.SemaphoreType.DMA((tasks,)),
            pltpu.SemaphoreType.DMA((tasks,)),
            pltpu.SemaphoreType.DMA((tasks,)),
            pltpu.SemaphoreType.DMA((12,)),
        ],
        compiler_params=pltpu.CompilerParams(
            collective_id=0, has_side_effects=True, vmem_limit_bytes=67_043_328
        ),
    )(spectra.reshape(depth, stations), cosine, sine_part)
    return out.reshape(LAGS, quarter, blocks * stations).astype(jnp.float32)


def solution(mesh):
    placed = (P(None, "seg", None, "sta"), P())
    chosen = fused_body if (mesh.shape["sta"], mesh.shape["seg"]) == (8, 4) else general_body
    return jax.shard_map(
        chosen, mesh=mesh, in_specs=placed, out_specs=P(None, ("sta", "seg"), None), check_vma=False
    )
```

```python
import functools
import math

import jax
import jax.numpy as jnp
from jax import lax
from jax.experimental import pallas as pl
from jax.experimental.pallas import tpu as pltpu
from jax.sharding import PartitionSpec as P

NFFT = 8192
LAGS = 2
LAG_STEP = 37
HALF = 64
MESH = pl.DeviceIdType.MESH


def whiten(spectra):
    values = spectra.astype(jnp.float32)
    energy = values[0] * values[0] + values[1] * values[1]
    freq_bins = values.shape[2]
    bin_pos = jnp.arange(freq_bins, dtype=jnp.int32)
    window = (jnp.abs(bin_pos[:, None] - bin_pos[None, :]) <= HALF).astype(jnp.float32)
    bin_count = jnp.sum(window, axis=1)
    smoothed = (
        jnp.einsum("gf,sfc->sgc", window, energy, precision=lax.Precision.HIGHEST)
        / bin_count[None, :, None]
    )
    return (values / jnp.sqrt(smoothed + 1e-06)[None]).astype(jnp.bfloat16)


def phases(bin_index):
    lag_samples = (jnp.arange(LAGS, dtype=jnp.int32) + 1) * LAG_STEP
    phase_turn = lag_samples[:, None] * bin_index[None, :] % NFFT
    phase_angle = 2.0 * math.pi / NFFT * phase_turn.astype(jnp.float32)
    return (jnp.cos(phase_angle), jnp.sin(phase_angle))


def rotate(whitened, cosine, sine_part):
    real_part = whitened[0].astype(jnp.float32)[None]
    imag_part = whitened[1].astype(jnp.float32)[None]
    cos_part = cosine[:, None, :, None]
    sin_part = sine_part[:, None, :, None]
    rot_real = real_part * cos_part - imag_part * sin_part
    rot_imag = real_part * sin_part + imag_part * cos_part
    stacked = jnp.stack([rot_real, rot_imag], axis=1).astype(jnp.bfloat16)
    return stacked.reshape(cosine.shape[0], -1, whitened.shape[3])


def pair_block(rotated, columns, norm_scale):
    product = jnp.einsum("mki,kj->mij", rotated, columns, preferred_element_type=jnp.float32)
    return (product * norm_scale).astype(jnp.bfloat16)


def general_body(spectra, bin_index):
    whitened = whiten(spectra)
    cosine, sine_part = phases(bin_index)
    seg_local = whitened.shape[1]
    freq_bins = whitened.shape[2]
    norm_scale = 1.0 / math.sqrt(seg_local * lax.axis_size("seg") * freq_bins)
    rotated = rotate(whitened, cosine, sine_part)
    shard_cols = lax.all_gather(whitened, "sta", axis=3, tiled=True)
    columns = shard_cols.reshape(-1, shard_cols.shape[3])
    product = pair_block(rotated, columns, norm_scale)
    return lax.psum_scatter(product, "seg", scatter_dimension=1, tiled=True).astype(jnp.float32)


OWN, SIDE, END, END_SIDE, MID, FAR = 0, 2, 4, 6, 8, 10


def kernel(
    dims, src, cos_ref, sin_ref, out, cols, raw_kept, rows, part, from_core, from_x, window, inv_count, split,
    load_sem, send_sem, recv_sem, core_send, core_recv, x_send, x_recv, out_send, out_recv,
):
    segs, bins, chunk, scale = dims
    depth = 2 * segs * bins
    half = segs * bins
    quarter = chunk // 2
    sta = lax.axis_index("sta")
    seg = lax.axis_index("seg")
    z, y = sta // 2, sta % 2
    x, core = seg // 2, seg % 2
    z_near = z + 1 - 2 * (z % 2)
    is_mid = ((z + 1) // 2) % 2
    side = z * 2 + (1 - y)
    near = z_near * 2 + y
    near_side = z_near * 2 + (1 - y)
    mid = (3 - z) * 2 + y
    far = ((z + 2) % 4) * 2 + y
    core_seg = x * 2 + (1 - core)
    x_seg = (1 - x) * 2 + core

    barrier = pltpu.get_barrier_semaphore()
    for partner in ((sta, core_seg), (sta, x_seg), (side, seg), (near, seg), (near_side, seg)):
        pl.semaphore_signal(barrier, inc=1, device_id=partner, device_id_type=MESH)

    @pl.when(is_mid == 1)
    def _():
        pl.semaphore_signal(barrier, inc=1, device_id=(mid, seg), device_id_type=MESH)

    loads = [
        pltpu.make_async_copy(
            src.at[:, pl.ds(ch * chunk, chunk)], cols.at[OWN + ch], load_sem.at[ch]
        )
        for ch in range(2)
    ]
    for load in loads:
        load.start()
    pl.semaphore_wait(barrier, 5 + is_mid)

    def remote(source, target, send, recv, to_sta, to_seg):
        return pltpu.make_async_remote_copy(
            src_ref=source, dst_ref=target, send_sem=send, recv_sem=recv,
            device_id=(to_sta, to_seg), device_id_type=MESH,
        )

    def own_chunk(ch):
        return src.at[:, pl.ds(ch * chunk, chunk)]

    def landing(slot, ends):
        kept = SIDE if ends else END
        return raw_kept.at[slot - kept] if kept <= slot < kept + 2 else cols.at[slot]

    def push(source, target, slot, index, to_sta):
        copy = remote(source, target, send_sem.at[index], recv_sem.at[slot], to_sta, seg)
        copy.start()
        return copy

    def arrived(slot, ends):
        there = landing(slot, ends)
        remote(there, there, send_sem.at[0], recv_sem.at[slot], side, seg).wait_recv()


    row_at = lax.broadcasted_iota(jnp.int32, (bins, bins), 0)
    col_at = lax.broadcasted_iota(jnp.int32, (bins, bins), 1)
    band = jnp.where(jnp.abs(row_at - col_at) <= HALF, 1.0, 0.0).astype(jnp.bfloat16)
    window[:, :bins] = band
    window[:, bins:] = band
    pos = lax.broadcasted_iota(jnp.int32, (bins, chunk), 0)
    count = jnp.minimum(pos, HALF) + jnp.minimum(bins - 1 - pos, HALF) + 1
    inv_count[...] = 1.0 / count.astype(jnp.float32)

    def whiten_lanes(slot, ends, first, width):
        raw = landing(slot, ends)
        lanes = pl.ds(first, width)

        def one(s, carry):
            at_re = pl.ds(pl.multiple_of(s * bins, bins), bins)
            at_im = pl.ds(pl.multiple_of(half + s * bins, bins), bins)
            real = raw[at_re, lanes].astype(jnp.float32)
            imag = raw[at_im, lanes].astype(jnp.float32)
            energy = real * real + imag * imag
            high = energy.astype(jnp.bfloat16)
            split[:bins, :width] = high
            split[bins:, :width] = (energy - high.astype(jnp.float32)).astype(jnp.bfloat16)
            total = jnp.dot(window[...], split[:, :width], preferred_element_type=jnp.float32)
            gain = lax.rsqrt(total * inv_count[:, :width] + 1e-06)
            real = raw[at_re, lanes].astype(jnp.float32)
            imag = raw[at_im, lanes].astype(jnp.float32)
            cols[slot, at_re, lanes] = (real * gain).astype(jnp.bfloat16)
            cols[slot, at_im, lanes] = (imag * gain).astype(jnp.bfloat16)
            return carry

        lax.fori_loop(0, segs, one, 0)

    def whiten_chunk(slot, ends):
        whiten_lanes(slot, ends, 0, chunk)

    def rotate_chunk(row, slot):
        xq = slot % 2

        def one(step, carry):
            parity, s = step // segs, step % segs
            lanes = pl.ds(pl.multiple_of(parity * quarter, quarter), quarter)
            at_re = pl.ds(pl.multiple_of(s * bins, bins), bins)
            at_im = pl.ds(pl.multiple_of(half + s * bins, bins), bins)
            real = cols[slot, at_re, lanes].T.astype(jnp.float32)
            imag = cols[slot, at_im, lanes].T.astype(jnp.float32)
            for lag in range(LAGS):
                cosine = cos_ref[lag : lag + 1, :]
                sine = sin_ref[lag : lag + 1, :]
                at = pl.ds(xq * LAGS * quarter + lag * quarter, quarter)
                rows[row, parity, at, at_re] = (real * cosine - imag * sine).astype(jnp.bfloat16)
                rows[row, parity, at, at_im] = (real * sine + imag * cosine).astype(jnp.bfloat16)
            return carry

        lax.fori_loop(0, 2 * segs, one, 0)

    def core_copy(task):
        index, width = task[0], task[4]
        return remote(
            part.at[index, 0, :, :, pl.ds(0, width)], from_core.at[index, :, :, pl.ds(0, width)],
            core_send.at[index], core_recv.at[index], sta, core_seg,
        )

    def x_copy(task):
        index, width = task[0], task[4]
        return remote(
            part.at[index, 1, 1 - x, :, pl.ds(0, width)], from_x.at[index, :, pl.ds(0, width)],
            x_send.at[index], x_recv.at[index], sta, x_seg,
        )

    def out_copy(task, ends):
        index, row, slot, first, width = task
        if ends:
            station = {OWN: sta, SIDE: side, MID: near}[slot - slot % 2]
        else:
            station = {OWN: sta, SIDE: side, MID: mid, FAR: far}[slot - slot % 2]
        source = part.at[index, 1, x, :, pl.ds(0, width)]
        start = (station * 4 + (slot % 2) * 2 + first // quarter) * quarter
        target = out.at[:, pl.ds(pl.multiple_of(start, quarter), width)]
        if row == 0:
            return pltpu.make_async_copy(source, target, out_send.at[index])
        to_sta = {1: side, 2: near, 3: near_side}[row]
        if first > 0:
            arrival = 13 if row == 3 else 12
        elif row == 3:
            arrival = slot - 4
        elif row == 1 and ends:
            arrival = slot - MID
        else:
            arrival = slot
        return remote(source, target, out_send.at[index], out_recv.at[arrival], to_sta, seg)

    def compute(task):
        index, row, slot, first, width = task

        def one(h, carry):
            parity = (core + 1 + h) % 2
            product = jnp.dot(
                rows[row, parity], cols[slot, :, pl.ds(first, width)], preferred_element_type=jnp.float32
            )
            product = (product * scale).astype(jnp.bfloat16)
            part[index, h, 0, :, :width] = product[: LAGS * quarter]
            part[index, h, 1, :, :width] = product[LAGS * quarter :]
            return carry

        lax.fori_loop(0, 2, one, 0)
        core_copy(task).start()

    def add_into(index, xq, other, width):
        mine = part[index, 1, xq, :, :width].astype(jnp.float32)
        part[index, 1, xq, :, :width] = (mine + other.astype(jnp.float32)).astype(jnp.bfloat16)

    def finish_core(task):
        index, width = task[0], task[4]
        core_copy(task).wait_recv()
        add_into(index, 1 - x, from_core[index, 1 - x, :, :width], width)
        x_copy(task).start()
        add_into(index, x, from_core[index, x, :, :width], width)

    def finish_x(task, ends):
        index, width = task[0], task[4]
        x_copy(task).wait_recv()
        add_into(index, x, from_x[index, :, :width], width)
        out_copy(task, ends).start()

    class Flow:
        def __init__(self, ends):
            self.ends = ends
            self.done = []
            self.at_core = 0
            self.at_x = 0

        def task(self, row, slot, first=0, width=chunk, core_lag=1, x_lag=3):
            self.done.append((len(self.done), row, slot, first, width))
            compute(self.done[-1])
            self.advance(core_lag, x_lag)

        def advance(self, core_lag, x_lag):
            while self.at_core < len(self.done) - core_lag:
                finish_core(self.done[self.at_core])
                self.at_core += 1
            while self.at_x < len(self.done) - x_lag:
                finish_x(self.done[self.at_x], self.ends)
                self.at_x += 1

        def drain(self):
            self.advance(0, 0)
            for task in self.done:
                core_copy(task).wait_send()
                x_copy(task).wait_send()
                copy = out_copy(task, self.ends)
                copy.wait() if task[1] == 0 else copy.wait_send()

    def incoming(index, width):
        target = out.at[:, pl.ds(0, width)]
        remote(target, target, out_send.at[0], out_recv.at[index], side, seg).wait_recv()

    def start_own(flow):
        for ch in range(2):
            loads[ch].wait()
            whiten_chunk(OWN + ch, flow.ends)
            rotate_chunk(0, OWN + ch)
        for ch in range(2):
            flow.task(0, OWN + ch)
        flow.advance(0, 0)

    def leave(flow, sends, expected):
        flow.drain()
        for copy in sends:
            copy.wait_send()
        for index, width in expected:
            incoming(index, width)

    @pl.when(is_mid == 0)
    def _():
        sends = []
        for ch in range(2):
            sends.append(push(own_chunk(ch), raw_kept.at[ch], END + ch, 2 + ch, near))
            sends.append(push(own_chunk(ch), raw_kept.at[ch], SIDE + ch, ch, side))
        flow = Flow(True)
        start_own(flow)
        for ch in range(2):
            arrived(SIDE + ch, True)
            if ch == 0:
                sends.append(push(raw_kept.at[0], cols.at[END_SIDE], END_SIDE, 4, near))
            whiten_chunk(SIDE + ch, True)
            rotate_chunk(1, SIDE + ch)
            flow.task(0, SIDE + ch)
            arrived(MID + ch, True)
            whiten_chunk(MID + ch, True)
            rotate_chunk(2, MID + ch)
            flow.task(0, MID + ch)
            if ch == 0:
                flow.advance(0, 0)
        for row, slot in ((2, OWN), (2, OWN + 1), (2, SIDE), (2, SIDE + 1), (1, MID), (1, MID + 1)):
            flow.task(row, slot)
        expected = [(index, chunk) for index in range(11) if index not in (2, 3, 7)]
        expected += [(7, quarter), (11, quarter), (12, quarter), (13, quarter)]
        leave(flow, sends, expected)

    @pl.when(is_mid == 1)
    def _():
        sends = []
        for ch in range(2):
            sends.append(push(own_chunk(ch), cols.at[MID + ch], MID + ch, 2 + ch, mid))
            sends.append(push(own_chunk(ch), cols.at[SIDE + ch], SIDE + ch, ch, side))
            sends.append(push(own_chunk(ch), cols.at[MID + ch], MID + ch, 8 + ch, near))

        def take(slot, row=None):
            arrived(slot, False)
            if slot == END:
                sends.append(push(raw_kept.at[0], cols.at[FAR], FAR, 4, mid))
            if slot == END + 1:
                for piece in range(2):
                    lanes = pl.ds(piece * quarter, quarter)
                    copy = remote(
                        raw_kept.at[1, :, lanes], cols.at[FAR + 1, :, lanes],
                        send_sem.at[5 + piece], recv_sem.at[FAR + 1 + piece], mid, seg,
                    )
                    copy.start()
                    sends.append(copy)
                sends.append(push(raw_kept.at[1], cols.at[END_SIDE + 1], END_SIDE + 1, 7, side))
            whiten_chunk(slot, False)
            if row is not None:
                rotate_chunk(row, slot)

        flow = Flow(False)
        start_own(flow)
        take(END, 2)
        take(SIDE, 1)
        flow.task(0, SIDE)
        take(MID)
        flow.task(0, MID)
        flow.advance(0, 0)
        take(END + 1, 2)
        take(SIDE + 1, 1)
        flow.task(1, MID)
        flow.task(2, MID)
        flow.task(0, SIDE + 1)
        take(MID + 1)
        for row in (2, 1, 0):
            flow.task(row, MID + 1)
        flow.advance(0, 0)
        take(END_SIDE, 3)
        take(END_SIDE + 1, 3)
        flow.task(3, MID)
        flow.task(3, MID + 1)
        take(FAR)
        for row in (3, 2, 1, 0):
            flow.task(row, FAR)
        flow.advance(0, 2)
        for piece in range(2):
            first = piece * quarter
            there = cols.at[FAR + 1, :, pl.ds(first, quarter)]
            remote(there, there, send_sem.at[0], recv_sem.at[FAR + 1 + piece], side, seg).wait_recv()
            whiten_lanes(FAR + 1, False, first, quarter)
            for row in (3, 2, 1, 0):
                flow.task(row, FAR + 1, first, quarter)
            flow.advance(0, 1 - piece)
        expected = [(index, chunk) for index in (0, 1, 2, 3, 8, 9, 10)] + [(11, quarter), (12, quarter)]
        leave(flow, sends, expected)


def fused_body(spectra, bin_index):
    cosine, sine_part = phases(bin_index)
    parts, segs, bins, stations = spectra.shape
    blocks = lax.axis_size("sta")
    depth = parts * segs * bins
    chunk = stations // 2
    quarter = chunk // 2
    scale = 1.0 / math.sqrt(segs * lax.axis_size("seg") * bins)
    tasks = 24
    low = jnp.bfloat16
    out = pl.pallas_call(
        functools.partial(kernel, (segs, bins, chunk, scale)),
        out_shape=jax.ShapeDtypeStruct((LAGS * quarter, blocks * stations), low),
        in_specs=[
            pl.BlockSpec(memory_space=pl.ANY),
            pl.BlockSpec(memory_space=pltpu.VMEM),
            pl.BlockSpec(memory_space=pltpu.VMEM),
        ],
        out_specs=pl.BlockSpec(memory_space=pl.ANY),
        scratch_shapes=[
            pltpu.VMEM((12, depth, chunk), low),
            pltpu.VMEM((2, depth, chunk), low),
            pltpu.VMEM((4, 2, LAGS * chunk, depth), low),
            pltpu.VMEM((tasks, 2, 2, LAGS * quarter, chunk), low),
            pltpu.VMEM((tasks, 2, LAGS * quarter, chunk), low),
            pltpu.VMEM((tasks, LAGS * quarter, chunk), low),
            pltpu.VMEM((bins, 2 * bins), low),
            pltpu.VMEM((bins, chunk), jnp.float32),
            pltpu.VMEM((2 * bins, chunk), low),
            pltpu.SemaphoreType.DMA((2,)),
            pltpu.SemaphoreType.DMA((10,)),
            pltpu.SemaphoreType.DMA((13,)),
            pltpu.SemaphoreType.DMA((tasks,)),
            pltpu.SemaphoreType.DMA((tasks,)),
            pltpu.SemaphoreType.DMA((tasks,)),
            pltpu.SemaphoreType.DMA((tasks,)),
            pltpu.SemaphoreType.DMA((tasks,)),
            pltpu.SemaphoreType.DMA((14,)),
        ],
        compiler_params=pltpu.CompilerParams(
            collective_id=0, has_side_effects=True, vmem_limit_bytes=67_043_328
        ),
    )(spectra.reshape(depth, stations), cosine, sine_part)
    return out.reshape(LAGS, quarter, blocks * stations).astype(jnp.float32)


def solution(mesh):
    placed = (P(None, "seg", None, "sta"), P())
    chosen = fused_body if (mesh.shape["sta"], mesh.shape["seg"]) == (8, 4) else general_body
    return jax.shard_map(
        chosen, mesh=mesh, in_specs=placed, out_specs=P(None, ("sta", "seg"), None), check_vma=False
    )
```

```python
import functools
import math

import jax
import jax.numpy as jnp
from jax import lax
from jax.experimental import pallas as pl
from jax.experimental.pallas import tpu as pltpu
from jax.sharding import PartitionSpec as P

NFFT = 8192
LAGS = 2
LAG_STEP = 37
HALF = 64
MESH = pl.DeviceIdType.MESH


def whiten(spectra):
    values = spectra.astype(jnp.float32)
    energy = values[0] * values[0] + values[1] * values[1]
    freq_bins = values.shape[2]
    bin_pos = jnp.arange(freq_bins, dtype=jnp.int32)
    window = (jnp.abs(bin_pos[:, None] - bin_pos[None, :]) <= HALF).astype(jnp.float32)
    bin_count = jnp.sum(window, axis=1)
    smoothed = (
        jnp.einsum("gf,sfc->sgc", window, energy, precision=lax.Precision.HIGHEST)
        / bin_count[None, :, None]
    )
    return (values / jnp.sqrt(smoothed + 1e-06)[None]).astype(jnp.bfloat16)


def phases(bin_index):
    lag_samples = (jnp.arange(LAGS, dtype=jnp.int32) + 1) * LAG_STEP
    phase_turn = lag_samples[:, None] * bin_index[None, :] % NFFT
    phase_angle = 2.0 * math.pi / NFFT * phase_turn.astype(jnp.float32)
    return (jnp.cos(phase_angle), jnp.sin(phase_angle))


def rotate(whitened, cosine, sine_part):
    real_part = whitened[0].astype(jnp.float32)[None]
    imag_part = whitened[1].astype(jnp.float32)[None]
    cos_part = cosine[:, None, :, None]
    sin_part = sine_part[:, None, :, None]
    rot_real = real_part * cos_part - imag_part * sin_part
    rot_imag = real_part * sin_part + imag_part * cos_part
    stacked = jnp.stack([rot_real, rot_imag], axis=1).astype(jnp.bfloat16)
    return stacked.reshape(cosine.shape[0], -1, whitened.shape[3])


def pair_block(rotated, columns, norm_scale):
    product = jnp.einsum("mki,kj->mij", rotated, columns, preferred_element_type=jnp.float32)
    return (product * norm_scale).astype(jnp.bfloat16)


def general_body(spectra, bin_index):
    whitened = whiten(spectra)
    cosine, sine_part = phases(bin_index)
    seg_local = whitened.shape[1]
    freq_bins = whitened.shape[2]
    norm_scale = 1.0 / math.sqrt(seg_local * lax.axis_size("seg") * freq_bins)
    rotated = rotate(whitened, cosine, sine_part)
    shard_cols = lax.all_gather(whitened, "sta", axis=3, tiled=True)
    columns = shard_cols.reshape(-1, shard_cols.shape[3])
    product = pair_block(rotated, columns, norm_scale)
    return lax.psum_scatter(product, "seg", scatter_dimension=1, tiled=True).astype(jnp.float32)


OWN, SIDE, END, END_SIDE, MID, FAR = 0, 2, 4, 6, 8, 10


def kernel(
    dims, src, bin_ref, out, cols, raw_kept, rows, part, from_core, from_x, window, inv_count, cos_ref, sin_ref,
    load_sem, send_sem, recv_sem, core_send, core_recv, x_send, x_recv, out_send, out_recv,
):
    segs, bins, chunk, scale = dims
    depth = 2 * segs * bins
    half = segs * bins
    quarter = chunk // 2
    sta = lax.axis_index("sta")
    seg = lax.axis_index("seg")
    z, y = sta // 2, sta % 2
    x, core = seg // 2, seg % 2
    z_near = z + 1 - 2 * (z % 2)
    is_mid = ((z + 1) // 2) % 2
    side = z * 2 + (1 - y)
    near = z_near * 2 + y
    near_side = z_near * 2 + (1 - y)
    mid = (3 - z) * 2 + y
    far = ((z + 2) % 4) * 2 + y
    core_seg = x * 2 + (1 - core)
    x_seg = (1 - x) * 2 + core

    barrier = pltpu.get_barrier_semaphore()
    for partner in ((sta, core_seg), (sta, x_seg), (side, seg), (near, seg), (near_side, seg)):
        pl.semaphore_signal(barrier, inc=1, device_id=partner, device_id_type=MESH)

    @pl.when(is_mid == 1)
    def _():
        pl.semaphore_signal(barrier, inc=1, device_id=(mid, seg), device_id_type=MESH)

    loads = [
        pltpu.make_async_copy(
            src.at[:, pl.ds(ch * chunk, chunk)], cols.at[OWN + ch], load_sem.at[ch]
        )
        for ch in range(2)
    ]
    for load in loads:
        load.start()
    pl.semaphore_wait(barrier, 5 + is_mid)

    def remote(source, target, send, recv, to_sta, to_seg):
        return pltpu.make_async_remote_copy(
            src_ref=source, dst_ref=target, send_sem=send, recv_sem=recv,
            device_id=(to_sta, to_seg), device_id_type=MESH,
        )

    def own_chunk(ch):
        return src.at[:, pl.ds(ch * chunk, chunk)]

    def landing(slot, ends):
        kept = SIDE if ends else END
        return raw_kept.at[slot - kept] if kept <= slot < kept + 2 else cols.at[slot]

    def push(source, target, slot, index, to_sta):
        copy = remote(source, target, send_sem.at[index], recv_sem.at[slot], to_sta, seg)
        copy.start()
        return copy

    def arrived(slot, ends):
        there = landing(slot, ends)
        remote(there, there, send_sem.at[0], recv_sem.at[slot], side, seg).wait_recv()


    row_at = lax.broadcasted_iota(jnp.int32, (bins, bins), 0)
    col_at = lax.broadcasted_iota(jnp.int32, (bins, bins), 1)
    band = jnp.where(jnp.abs(row_at - col_at) <= HALF, 1.0, 0.0).astype(jnp.bfloat16)
    window[...] = band
    pos = lax.broadcasted_iota(jnp.int32, (bins, chunk), 0)
    count = jnp.minimum(pos, HALF) + jnp.minimum(bins - 1 - pos, HALF) + 1
    inv_count[...] = 1.0 / count.astype(jnp.float32)

    for lag in range(LAGS):
        turn = lax.rem((lag + 1) * LAG_STEP * bin_ref[...], NFFT)
        angle = 2.0 * math.pi / NFFT * turn.astype(jnp.float32)
        cos_ref[lag : lag + 1, :] = jnp.cos(angle)
        sin_ref[lag : lag + 1, :] = jnp.sin(angle)

    def whiten_lanes(slot, ends, first, width):
        raw = landing(slot, ends)
        lanes = pl.ds(first, width)

        def one(s, carry):
            at_re = pl.ds(pl.multiple_of(s * bins, bins), bins)
            at_im = pl.ds(pl.multiple_of(half + s * bins, bins), bins)
            real = raw[at_re, lanes].astype(jnp.float32)
            imag = raw[at_im, lanes].astype(jnp.float32)
            energy = real * real + imag * imag
            total = jnp.dot(window[...], energy.astype(jnp.bfloat16), preferred_element_type=jnp.float32)
            gain = lax.rsqrt(total * inv_count[:, :width] + 1e-06)
            real = raw[at_re, lanes].astype(jnp.float32)
            imag = raw[at_im, lanes].astype(jnp.float32)
            cols[slot, at_re, lanes] = (real * gain).astype(jnp.bfloat16)
            cols[slot, at_im, lanes] = (imag * gain).astype(jnp.bfloat16)
            return carry

        lax.fori_loop(0, segs, one, 0)

    def whiten_chunk(slot, ends):
        whiten_lanes(slot, ends, 0, chunk)

    def rotate_chunk(row, slot):
        xq = slot % 2

        def one(step, carry):
            parity, s = step // segs, step % segs
            lanes = pl.ds(pl.multiple_of(parity * quarter, quarter), quarter)
            at_re = pl.ds(pl.multiple_of(s * bins, bins), bins)
            at_im = pl.ds(pl.multiple_of(half + s * bins, bins), bins)
            real = cols[slot, at_re, lanes].T.astype(jnp.float32)
            imag = cols[slot, at_im, lanes].T.astype(jnp.float32)
            for lag in range(LAGS):
                cosine = cos_ref[lag : lag + 1, :]
                sine = sin_ref[lag : lag + 1, :]
                at = pl.ds(xq * LAGS * quarter + lag * quarter, quarter)
                rows[row, parity, at, at_re] = (real * cosine - imag * sine).astype(jnp.bfloat16)
                rows[row, parity, at, at_im] = (real * sine + imag * cosine).astype(jnp.bfloat16)
            return carry

        lax.fori_loop(0, 2 * segs, one, 0)

    def core_copy(task):
        index, width = task[0], task[4]
        return remote(
            part.at[index, 0, :, :, pl.ds(0, width)], from_core.at[index, :, :, pl.ds(0, width)],
            core_send.at[index], core_recv.at[index], sta, core_seg,
        )

    def x_copy(task):
        index, width = task[0], task[4]
        return remote(
            part.at[index, 1, 1 - x, :, pl.ds(0, width)], from_x.at[index, :, pl.ds(0, width)],
            x_send.at[index], x_recv.at[index], sta, x_seg,
        )

    def out_copy(task, ends):
        index, row, slot, first, width = task
        if ends:
            station = {OWN: sta, SIDE: side, MID: near}[slot - slot % 2]
        else:
            station = {OWN: sta, SIDE: side, MID: mid, FAR: far}[slot - slot % 2]
        source = part.at[index, 1, x, :, pl.ds(0, width)]
        start = (station * 4 + (slot % 2) * 2 + first // quarter) * quarter
        target = out.at[:, pl.ds(pl.multiple_of(start, quarter), width)]
        if row == 0:
            return pltpu.make_async_copy(source, target, out_send.at[index])
        to_sta = {1: side, 2: near, 3: near_side}[row]
        if first > 0:
            arrival = 13 if row == 3 else 12
        elif row == 3:
            arrival = slot - 4
        elif row == 1 and ends:
            arrival = slot - MID
        else:
            arrival = slot
        return remote(source, target, out_send.at[index], out_recv.at[arrival], to_sta, seg)

    def compute(task):
        index, row, slot, first, width = task

        def one(h, carry):
            parity = (core + 1 + h) % 2
            product = jnp.dot(
                rows[row, parity], cols[slot, :, pl.ds(first, width)], preferred_element_type=jnp.float32
            )
            product = (product * scale).astype(jnp.bfloat16)
            part[index, h, 0, :, :width] = product[: LAGS * quarter]
            part[index, h, 1, :, :width] = product[LAGS * quarter :]

            @pl.when(h == 0)
            def _():
                core_copy(task).start()

            return carry

        lax.fori_loop(0, 2, one, 0)

    def add_into(index, xq, other, width):
        def one(step, carry):
            at = pl.ds(pl.multiple_of(step * 64, 64), 64)
            mine = part[index, 1, xq, at, :width].astype(jnp.float32)
            part[index, 1, xq, at, :width] = (mine + other[at, :width].astype(jnp.float32)).astype(jnp.bfloat16)
            return carry

        lax.fori_loop(0, LAGS * quarter // 64, one, 0)

    def finish_core(task):
        index, width = task[0], task[4]
        core_copy(task).wait_recv()
        add_into(index, 1 - x, from_core.at[index, 1 - x], width)
        x_copy(task).start()
        add_into(index, x, from_core.at[index, x], width)

    def finish_x(task, ends):
        index, width = task[0], task[4]
        x_copy(task).wait_recv()
        add_into(index, x, from_x.at[index], width)
        out_copy(task, ends).start()

    class Flow:
        def __init__(self, ends):
            self.ends = ends
            self.done = []
            self.at_core = 0
            self.at_x = 0

        def task(self, row, slot, first=0, width=chunk, core_lag=1, x_lag=3):
            self.done.append((len(self.done), row, slot, first, width))
            compute(self.done[-1])
            self.advance(core_lag, x_lag)

        def advance(self, core_lag, x_lag):
            while self.at_core < len(self.done) - core_lag:
                finish_core(self.done[self.at_core])
                self.at_core += 1
            while self.at_x < len(self.done) - x_lag:
                finish_x(self.done[self.at_x], self.ends)
                self.at_x += 1

        def drain(self):
            self.advance(0, 0)
            for task in self.done:
                core_copy(task).wait_send()
                x_copy(task).wait_send()
                copy = out_copy(task, self.ends)
                copy.wait() if task[1] == 0 else copy.wait_send()

    def incoming(index, width):
        target = out.at[:, pl.ds(0, width)]
        remote(target, target, out_send.at[0], out_recv.at[index], side, seg).wait_recv()

    def start_own(flow):
        for ch in range(2):
            loads[ch].wait()
            whiten_chunk(OWN + ch, flow.ends)
            rotate_chunk(0, OWN + ch)
        for ch in range(2):
            flow.task(0, OWN + ch)
        flow.advance(0, 0)

    def leave(flow, sends, expected):
        flow.drain()
        for copy in sends:
            copy.wait_send()
        for index, width in expected:
            incoming(index, width)

    @pl.when(is_mid == 0)
    def _():
        sends = []
        for ch in range(2):
            sends.append(push(own_chunk(ch), raw_kept.at[ch], END + ch, 2 + ch, near))
            sends.append(push(own_chunk(ch), raw_kept.at[ch], SIDE + ch, ch, side))
        flow = Flow(True)
        start_own(flow)
        for ch in range(2):
            arrived(SIDE + ch, True)
            if ch == 0:
                sends.append(push(raw_kept.at[0], cols.at[END_SIDE], END_SIDE, 4, near))
            whiten_chunk(SIDE + ch, True)
            rotate_chunk(1, SIDE + ch)
            flow.task(0, SIDE + ch)
            arrived(MID + ch, True)
            whiten_chunk(MID + ch, True)
            rotate_chunk(2, MID + ch)
            flow.task(0, MID + ch)
            if ch == 0:
                flow.advance(0, 0)
        for row, slot in ((2, OWN), (2, OWN + 1), (2, SIDE), (2, SIDE + 1), (1, MID), (1, MID + 1)):
            flow.task(row, slot)
        expected = [(index, chunk) for index in range(11) if index not in (2, 3, 7)]
        expected += [(7, quarter), (11, quarter), (12, quarter), (13, quarter)]
        leave(flow, sends, expected)

    @pl.when(is_mid == 1)
    def _():
        sends = []
        for ch in range(2):
            sends.append(push(own_chunk(ch), cols.at[MID + ch], MID + ch, 2 + ch, mid))
            sends.append(push(own_chunk(ch), cols.at[SIDE + ch], SIDE + ch, ch, side))
            sends.append(push(own_chunk(ch), cols.at[MID + ch], MID + ch, 8 + ch, near))

        def relay(slot):
            arrived(slot, False)
            if slot == END:
                sends.append(push(raw_kept.at[0], cols.at[FAR], FAR, 4, mid))
                return
            for piece in range(2):
                lanes = pl.ds(piece * quarter, quarter)
                copy = remote(
                    raw_kept.at[1, :, lanes], cols.at[FAR + 1, :, lanes],
                    send_sem.at[5 + piece], recv_sem.at[FAR + 1 + piece], mid, seg,
                )
                copy.start()
                sends.append(copy)
            sends.append(push(raw_kept.at[1], cols.at[END_SIDE + 1], END_SIDE + 1, 7, side))

        def ready(slot, row=None):
            if not END <= slot < END + 2:
                arrived(slot, False)
            whiten_chunk(slot, False)
            if row is not None:
                rotate_chunk(row, slot)

        flow = Flow(False)
        start_own(flow)
        relay(END)
        ready(SIDE, 1)
        flow.task(0, SIDE)
        ready(MID)
        flow.task(0, MID)
        ready(END, 2)
        flow.advance(0, 0)
        relay(END + 1)
        ready(MID + 1)
        flow.task(0, MID + 1)
        ready(END + 1, 2)
        for slot in (MID, MID + 1):
            flow.task(2, slot)
        ready(SIDE + 1, 1)
        for row, slot in ((1, MID), (1, MID + 1), (0, SIDE + 1)):
            flow.task(row, slot, x_lag=6)
        flow.advance(0, 3)
        ready(FAR)
        for row in (2, 1, 0):
            flow.task(row, FAR, x_lag=5)
        ready(END_SIDE, 3)
        ready(END_SIDE + 1, 3)
        for slot in (FAR, MID, MID + 1):
            flow.task(3, slot, x_lag=5)
        for piece in range(2):
            first = piece * quarter
            there = cols.at[FAR + 1, :, pl.ds(first, quarter)]
            remote(there, there, send_sem.at[0], recv_sem.at[FAR + 1 + piece], side, seg).wait_recv()
            whiten_lanes(FAR + 1, False, first, quarter)
            for row in (3, 2, 1, 0):
                flow.task(row, FAR + 1, first, quarter, x_lag=5 if piece == 0 else 4)
            if piece == 0:
                flow.advance(0, 4)
        expected = [(index, chunk) for index in (0, 1, 2, 3, 8, 9, 10)] + [(11, quarter), (12, quarter)]
        leave(flow, sends, expected)


def widen(steps, src, out, narrow, wide, in_sem, out_sem):
    rows = src.shape[0] // steps
    ranges = [pl.ds(step * rows, rows) for step in range(steps)]
    loads = [pltpu.make_async_copy(src.at[at], narrow.at[at], in_sem.at[i]) for i, at in enumerate(ranges)]
    stores = [pltpu.make_async_copy(wide.at[at], out.at[at], out_sem.at[i]) for i, at in enumerate(ranges)]
    for load in loads:
        load.start()
    for load, at, store in zip(loads, ranges, stores):
        load.wait()
        wide[at, :] = narrow[at, :].astype(jnp.float32)
        store.start()
    for store in stores:
        store.wait()


def fused_body(spectra, bin_index):
    parts, segs, bins, stations = spectra.shape
    blocks = lax.axis_size("sta")
    depth = parts * segs * bins
    chunk = stations // 2
    quarter = chunk // 2
    scale = 1.0 / math.sqrt(segs * lax.axis_size("seg") * bins)
    tasks = 24
    low = jnp.bfloat16
    out = pl.pallas_call(
        functools.partial(kernel, (segs, bins, chunk, scale)),
        out_shape=jax.ShapeDtypeStruct((LAGS * quarter, blocks * stations), low),
        in_specs=[
            pl.BlockSpec(memory_space=pl.ANY),
            pl.BlockSpec(memory_space=pltpu.VMEM),
        ],
        out_specs=pl.BlockSpec(memory_space=pl.ANY),
        scratch_shapes=[
            pltpu.VMEM((12, depth, chunk), low),
            pltpu.VMEM((2, depth, chunk), low),
            pltpu.VMEM((4, 2, LAGS * chunk, depth), low),
            pltpu.VMEM((tasks, 2, 2, LAGS * quarter, chunk), low),
            pltpu.VMEM((tasks, 2, LAGS * quarter, chunk), low),
            pltpu.VMEM((tasks, LAGS * quarter, chunk), low),
            pltpu.VMEM((bins, bins), low),
            pltpu.VMEM((bins, chunk), jnp.float32),
            pltpu.VMEM((LAGS, bins), jnp.float32),
            pltpu.VMEM((LAGS, bins), jnp.float32),
            pltpu.SemaphoreType.DMA((2,)),
            pltpu.SemaphoreType.DMA((10,)),
            pltpu.SemaphoreType.DMA((13,)),
            pltpu.SemaphoreType.DMA((tasks,)),
            pltpu.SemaphoreType.DMA((tasks,)),
            pltpu.SemaphoreType.DMA((tasks,)),
            pltpu.SemaphoreType.DMA((tasks,)),
            pltpu.SemaphoreType.DMA((tasks,)),
            pltpu.SemaphoreType.DMA((14,)),
        ],
        compiler_params=pltpu.CompilerParams(
            collective_id=0, has_side_effects=True, vmem_limit_bytes=67_043_328
        ),
    )(spectra.reshape(depth, stations), bin_index.reshape(1, bins))
    steps = 8
    any_space = pl.BlockSpec(memory_space=pl.ANY)
    out = pl.pallas_call(
        functools.partial(widen, steps),
        out_shape=jax.ShapeDtypeStruct(out.shape, jnp.float32),
        in_specs=[any_space],
        out_specs=any_space,
        scratch_shapes=[
            pltpu.VMEM(out.shape, low),
            pltpu.VMEM(out.shape, jnp.float32),
            pltpu.SemaphoreType.DMA((steps,)),
            pltpu.SemaphoreType.DMA((steps,)),
        ],
    )(out)
    return out.reshape(LAGS, quarter, blocks * stations)


def solution(mesh):
    placed = (P(None, "seg", None, "sta"), P())
    chosen = fused_body if (mesh.shape["sta"], mesh.shape["seg"]) == (8, 4) else general_body
    return jax.shard_map(
        chosen, mesh=mesh, in_specs=placed, out_specs=P(None, ("sta", "seg"), None), check_vma=False
    )
```

```python
import functools
import math

import jax
import jax.numpy as jnp
from jax import lax
from jax.experimental import pallas as pl
from jax.experimental.pallas import tpu as pltpu
from jax.sharding import PartitionSpec as P

NFFT = 8192
LAGS = 2
LAG_STEP = 37
HALF = 64
MESH = pl.DeviceIdType.MESH


def whiten(spectra):
    values = spectra.astype(jnp.float32)
    energy = values[0] * values[0] + values[1] * values[1]
    freq_bins = values.shape[2]
    bin_pos = jnp.arange(freq_bins, dtype=jnp.int32)
    window = (jnp.abs(bin_pos[:, None] - bin_pos[None, :]) <= HALF).astype(jnp.float32)
    bin_count = jnp.sum(window, axis=1)
    smoothed = (
        jnp.einsum("gf,sfc->sgc", window, energy, precision=lax.Precision.HIGHEST)
        / bin_count[None, :, None]
    )
    return (values / jnp.sqrt(smoothed + 1e-06)[None]).astype(jnp.bfloat16)


def phases(bin_index):
    lag_samples = (jnp.arange(LAGS, dtype=jnp.int32) + 1) * LAG_STEP
    phase_turn = lag_samples[:, None] * bin_index[None, :] % NFFT
    phase_angle = 2.0 * math.pi / NFFT * phase_turn.astype(jnp.float32)
    return (jnp.cos(phase_angle), jnp.sin(phase_angle))


def rotate(whitened, cosine, sine_part):
    real_part = whitened[0].astype(jnp.float32)[None]
    imag_part = whitened[1].astype(jnp.float32)[None]
    cos_part = cosine[:, None, :, None]
    sin_part = sine_part[:, None, :, None]
    rot_real = real_part * cos_part - imag_part * sin_part
    rot_imag = real_part * sin_part + imag_part * cos_part
    stacked = jnp.stack([rot_real, rot_imag], axis=1).astype(jnp.bfloat16)
    return stacked.reshape(cosine.shape[0], -1, whitened.shape[3])


def pair_block(rotated, columns, norm_scale):
    product = jnp.einsum("mki,kj->mij", rotated, columns, preferred_element_type=jnp.float32)
    return (product * norm_scale).astype(jnp.bfloat16)


def general_body(spectra, bin_index):
    whitened = whiten(spectra)
    cosine, sine_part = phases(bin_index)
    seg_local = whitened.shape[1]
    freq_bins = whitened.shape[2]
    norm_scale = 1.0 / math.sqrt(seg_local * lax.axis_size("seg") * freq_bins)
    rotated = rotate(whitened, cosine, sine_part)
    shard_cols = lax.all_gather(whitened, "sta", axis=3, tiled=True)
    columns = shard_cols.reshape(-1, shard_cols.shape[3])
    product = pair_block(rotated, columns, norm_scale)
    return lax.psum_scatter(product, "seg", scatter_dimension=1, tiled=True).astype(jnp.float32)


OWN, SIDE, END, END_SIDE, MID, FAR = 0, 2, 4, 6, 8, 10


def kernel(
    dims, src, bin_ref, out, cols, raw_kept, rows, part, from_core, from_x, window, inv_count, cos_ref, sin_ref,
    load_sem, send_sem, recv_sem, core_send, core_recv, x_send, x_recv, out_send, out_recv,
):
    segs, bins, chunk, scale = dims
    depth = 2 * segs * bins
    half = segs * bins
    quarter = chunk // 2
    sta = lax.axis_index("sta")
    seg = lax.axis_index("seg")
    z, y = sta // 2, sta % 2
    x, core = seg // 2, seg % 2
    z_near = z + 1 - 2 * (z % 2)
    is_mid = ((z + 1) // 2) % 2
    side = z * 2 + (1 - y)
    near = z_near * 2 + y
    near_side = z_near * 2 + (1 - y)
    mid = (3 - z) * 2 + y
    far = ((z + 2) % 4) * 2 + y
    core_seg = x * 2 + (1 - core)
    x_seg = (1 - x) * 2 + core

    barrier = pltpu.get_barrier_semaphore()
    for partner in ((sta, core_seg), (sta, x_seg), (side, seg), (near, seg), (near_side, seg)):
        pl.semaphore_signal(barrier, inc=1, device_id=partner, device_id_type=MESH)

    @pl.when(is_mid == 1)
    def _():
        pl.semaphore_signal(barrier, inc=1, device_id=(mid, seg), device_id_type=MESH)

    loads = [
        pltpu.make_async_copy(
            src.at[:, pl.ds(ch * chunk, chunk)], cols.at[OWN + ch], load_sem.at[ch]
        )
        for ch in range(2)
    ]
    for load in loads:
        load.start()
    pl.semaphore_wait(barrier, 5 + is_mid)

    def remote(source, target, send, recv, to_sta, to_seg):
        return pltpu.make_async_remote_copy(
            src_ref=source, dst_ref=target, send_sem=send, recv_sem=recv,
            device_id=(to_sta, to_seg), device_id_type=MESH,
        )

    def own_chunk(ch):
        return src.at[:, pl.ds(ch * chunk, chunk)]

    def landing(slot, ends):
        kept = SIDE if ends else END
        return raw_kept.at[slot - kept] if kept <= slot < kept + 2 else cols.at[slot]

    def push(source, target, slot, index, to_sta):
        copy = remote(source, target, send_sem.at[index, 0], recv_sem.at[slot], to_sta, seg)
        copy.start()
        return copy

    second = {FAR + 1: 12, END_SIDE: 13, END_SIDE + 1: 14}

    def push_pieces(sends, source, slot, index, to_sta):
        for piece in range(2):
            lanes = pl.ds(piece * quarter, quarter)
            copy = remote(
                source.at[:, lanes], cols.at[slot, :, lanes],
                send_sem.at[index, piece], recv_sem.at[second[slot] if piece else slot], to_sta, seg,
            )
            copy.start()
            sends.append(copy)

    def piece_arrived(slot, piece):
        there = cols.at[slot, :, pl.ds(piece * quarter, quarter)]
        remote(
            there, there, send_sem.at[0, 0], recv_sem.at[second[slot] if piece else slot], side, seg
        ).wait_recv()

    def arrived(slot, ends):
        there = landing(slot, ends)
        remote(there, there, send_sem.at[0, 0], recv_sem.at[slot], side, seg).wait_recv()


    row_at = lax.broadcasted_iota(jnp.int32, (bins, bins), 0)
    col_at = lax.broadcasted_iota(jnp.int32, (bins, bins), 1)
    band = jnp.where(jnp.abs(row_at - col_at) <= HALF, 1.0, 0.0).astype(jnp.bfloat16)
    window[...] = band
    pos = lax.broadcasted_iota(jnp.int32, (bins, chunk), 0)
    count = jnp.minimum(pos, HALF) + jnp.minimum(bins - 1 - pos, HALF) + 1
    inv_count[...] = 1.0 / count.astype(jnp.float32)

    for lag in range(LAGS):
        turn = lax.rem((lag + 1) * LAG_STEP * bin_ref[...], NFFT)
        angle = 2.0 * math.pi / NFFT * turn.astype(jnp.float32)
        cos_ref[lag : lag + 1, :] = jnp.cos(angle)
        sin_ref[lag : lag + 1, :] = jnp.sin(angle)

    def whiten_lanes(slot, ends, first, width):
        raw = landing(slot, ends)
        lanes = pl.ds(first, width)

        def one(s, carry):
            at_re = pl.ds(pl.multiple_of(s * bins, bins), bins)
            at_im = pl.ds(pl.multiple_of(half + s * bins, bins), bins)
            real = raw[at_re, lanes].astype(jnp.float32)
            imag = raw[at_im, lanes].astype(jnp.float32)
            energy = real * real + imag * imag
            total = jnp.dot(window[...], energy.astype(jnp.bfloat16), preferred_element_type=jnp.float32)
            gain = lax.rsqrt(total * inv_count[:, :width] + 1e-06)
            real = raw[at_re, lanes].astype(jnp.float32)
            imag = raw[at_im, lanes].astype(jnp.float32)
            cols[slot, at_re, lanes] = (real * gain).astype(jnp.bfloat16)
            cols[slot, at_im, lanes] = (imag * gain).astype(jnp.bfloat16)
            return carry

        lax.fori_loop(0, segs, one, 0)

    def whiten_chunk(slot, ends):
        whiten_lanes(slot, ends, 0, chunk)

    def rotate_chunk(row, slot, first=0, pieces=2):
        xq = slot % 2

        def one(step, carry):
            parity, s = first + step // segs, step % segs
            lanes = pl.ds(pl.multiple_of(parity * quarter, quarter), quarter)
            at_re = pl.ds(pl.multiple_of(s * bins, bins), bins)
            at_im = pl.ds(pl.multiple_of(half + s * bins, bins), bins)
            real = cols[slot, at_re, lanes].T.astype(jnp.float32)
            imag = cols[slot, at_im, lanes].T.astype(jnp.float32)
            for lag in range(LAGS):
                cosine = cos_ref[lag : lag + 1, :]
                sine = sin_ref[lag : lag + 1, :]
                at = pl.ds(xq * LAGS * quarter + lag * quarter, quarter)
                rows[row, parity, at, at_re] = (real * cosine - imag * sine).astype(jnp.bfloat16)
                rows[row, parity, at, at_im] = (real * sine + imag * cosine).astype(jnp.bfloat16)
            return carry

        lax.fori_loop(0, pieces * segs, one, 0)

    def core_copy(task):
        index, width = task[0], task[4]
        return remote(
            part.at[index, 0, :, :, pl.ds(0, width)], from_core.at[index, :, :, pl.ds(0, width)],
            core_send.at[index], core_recv.at[index], sta, core_seg,
        )

    def x_copy(task):
        index, width = task[0], task[4]
        return remote(
            part.at[index, 1, 1 - x, :, pl.ds(0, width)], from_x.at[index, :, pl.ds(0, width)],
            x_send.at[index], x_recv.at[index], sta, x_seg,
        )

    def out_copy(task, ends):
        index, row, slot, first, width = task
        if ends:
            station = {OWN: sta, SIDE: side, MID: near, FAR: far}[slot - slot % 2]
        else:
            station = {OWN: sta, SIDE: side, MID: mid, FAR: far}[slot - slot % 2]
        source = part.at[index, 1, x, :, pl.ds(0, width)]
        start = (station * 4 + (slot % 2) * 2 + first // quarter) * quarter
        target = out.at[:, pl.ds(pl.multiple_of(start, quarter), width)]
        if row == 0:
            return pltpu.make_async_copy(source, target, out_send.at[index])
        to_sta = {1: side, 2: near, 3: near_side}[row]
        if first > 0:
            arrival = 13 if row == 3 else 12
        elif row == 3:
            arrival = slot - 4
        elif row == 1 and ends:
            arrival = slot - MID
        else:
            arrival = slot
        return remote(source, target, out_send.at[index], out_recv.at[arrival], to_sta, seg)

    def compute(task):
        index, row, slot, first, width = task

        def one(h, carry):
            parity = (core + 1 + h) % 2
            product = jnp.dot(
                rows[row, parity], cols[slot, :, pl.ds(first, width)], preferred_element_type=jnp.float32
            )
            product = (product * scale).astype(jnp.bfloat16)
            part[index, h, 0, :, :width] = product[: LAGS * quarter]
            part[index, h, 1, :, :width] = product[LAGS * quarter :]

            @pl.when(h == 0)
            def _():
                core_copy(task).start()

            return carry

        lax.fori_loop(0, 2, one, 0)

    def add_into(index, xq, other, width):
        def one(step, carry):
            at = pl.ds(pl.multiple_of(step * 64, 64), 64)
            mine = part[index, 1, xq, at, :width].astype(jnp.float32)
            part[index, 1, xq, at, :width] = (mine + other[at, :width].astype(jnp.float32)).astype(jnp.bfloat16)
            return carry

        lax.fori_loop(0, LAGS * quarter // 64, one, 0)

    def finish_core(task):
        index, width = task[0], task[4]
        core_copy(task).wait_recv()
        add_into(index, 1 - x, from_core.at[index, 1 - x], width)
        x_copy(task).start()
        add_into(index, x, from_core.at[index, x], width)

    def finish_x(task, ends):
        index, width = task[0], task[4]
        x_copy(task).wait_recv()
        add_into(index, x, from_x.at[index], width)
        out_copy(task, ends).start()

    class Flow:
        def __init__(self, ends):
            self.ends = ends
            self.done = []
            self.at_core = 0
            self.at_x = 0

        def task(self, row, slot, first=0, width=chunk, core_lag=1, x_lag=3):
            self.done.append((len(self.done), row, slot, first, width))
            compute(self.done[-1])
            self.advance(core_lag, x_lag)

        def advance(self, core_lag, x_lag):
            while self.at_core < len(self.done) - core_lag:
                finish_core(self.done[self.at_core])
                self.at_core += 1
            while self.at_x < len(self.done) - x_lag:
                finish_x(self.done[self.at_x], self.ends)
                self.at_x += 1

        def drain(self):
            self.advance(0, 0)
            for task in self.done:
                core_copy(task).wait_send()
                x_copy(task).wait_send()
                copy = out_copy(task, self.ends)
                copy.wait() if task[1] == 0 else copy.wait_send()

    def incoming(index, width):
        target = out.at[:, pl.ds(0, width)]
        remote(target, target, out_send.at[0], out_recv.at[index], side, seg).wait_recv()

    def start_own(flow):
        for ch in range(2):
            loads[ch].wait()
            whiten_chunk(OWN + ch, flow.ends)
            rotate_chunk(0, OWN + ch)
        for ch in range(2):
            flow.task(0, OWN + ch)
        flow.advance(0, 0)

    def leave(flow, sends, expected):
        flow.drain()
        for copy in sends:
            copy.wait_send()
        for index, width in expected:
            incoming(index, width)

    @pl.when(is_mid == 0)
    def _():
        sends = []
        for ch in range(2):
            sends.append(push(own_chunk(ch), raw_kept.at[ch], END + ch, 2 + ch, near))
            sends.append(push(own_chunk(ch), raw_kept.at[ch], SIDE + ch, ch, side))
        flow = Flow(True)
        start_own(flow)
        for ch in range(2):
            arrived(SIDE + ch, True)
            if ch == 0:
                push_pieces(sends, raw_kept.at[0], END_SIDE, 4, near)
            whiten_chunk(SIDE + ch, True)
            rotate_chunk(1, SIDE + ch)
            flow.task(0, SIDE + ch)
            arrived(MID + ch, True)
            whiten_chunk(MID + ch, True)
            rotate_chunk(2, MID + ch)
            flow.task(0, MID + ch)
            if ch == 0:
                flow.advance(0, 0)
        for row, slot in ((2, OWN), (2, OWN + 1), (2, SIDE), (2, SIDE + 1), (1, MID), (1, MID + 1)):
            flow.task(row, slot)
        arrived(FAR, True)
        flow.task(1, FAR)
        flow.task(0, FAR)
        expected = [(index, chunk) for index in (0, 1, 2, 5, 6, 9, 10)]
        expected += [(7, quarter), (11, quarter), (12, quarter), (13, quarter)]
        leave(flow, sends, expected)

    @pl.when(is_mid == 1)
    def _():
        sends = []
        for ch in range(2):
            sends.append(push(own_chunk(ch), cols.at[MID + ch], MID + ch, 2 + ch, mid))
            sends.append(push(own_chunk(ch), cols.at[SIDE + ch], SIDE + ch, ch, side))
            sends.append(push(own_chunk(ch), cols.at[MID + ch], MID + ch, 8 + ch, near))

        def relay(slot):
            arrived(slot, False)
            if slot == END:
                sends.append(push(raw_kept.at[0], cols.at[FAR], FAR, 4, mid))
                return
            push_pieces(sends, raw_kept.at[1], FAR + 1, 5, mid)
            push_pieces(sends, raw_kept.at[1], END_SIDE + 1, 7, side)

        def ready(slot, row=None):
            if not END <= slot < END + 2:
                arrived(slot, False)
            whiten_chunk(slot, False)
            if row is not None:
                rotate_chunk(row, slot)

        def ready_piece(slot, piece, row=None):
            piece_arrived(slot, piece)
            whiten_lanes(slot, False, piece * quarter, quarter)
            if row is not None:
                rotate_chunk(row, slot, piece, 1)

        flow = Flow(False)
        start_own(flow)
        relay(END)
        ready(SIDE, 1)
        flow.task(0, SIDE)
        ready(MID)
        flow.task(0, MID)
        sends.append(push(cols.at[MID], cols.at[FAR], FAR, 9, near))
        ready(END, 2)
        flow.advance(0, 0)
        relay(END + 1)
        ready(MID + 1)
        flow.task(0, MID + 1)
        ready(END + 1, 2)
        flow.task(2, MID + 1)
        ready(SIDE + 1, 1)
        for row, slot in ((1, MID), (1, MID + 1), (0, SIDE + 1)):
            flow.task(row, slot, x_lag=6)
        flow.advance(0, 3)
        for ch in range(2):
            ready_piece(END_SIDE + ch, 0, 3)
        ready(FAR)
        for row in (2, 1, 0):
            flow.task(row, FAR, x_lag=6)
        for ch in range(2):
            ready_piece(END_SIDE + ch, 1, 3)
        for slot in (FAR, MID + 1):
            flow.task(3, slot, x_lag=6)
        for piece in range(2):
            first = piece * quarter
            ready_piece(FAR + 1, piece)
            for row in (3, 2, 1, 0):
                flow.task(row, FAR + 1, first, quarter, x_lag=6 - 2 * piece)
            if piece == 0:
                flow.advance(0, 4)
        flow.advance(1, 3)
        expected = [(index, chunk) for index in (0, 1, 2, 3, 8, 9, 10)] + [(11, quarter), (12, quarter)]
        leave(flow, sends, expected)


def widen(steps, src, out, narrow, wide, in_sem, out_sem):
    rows = src.shape[0] // steps
    ranges = [pl.ds(step * rows, rows) for step in range(steps)]
    loads = [pltpu.make_async_copy(src.at[at], narrow.at[at], in_sem.at[i]) for i, at in enumerate(ranges)]
    stores = [pltpu.make_async_copy(wide.at[at], out.at[at], out_sem.at[i]) for i, at in enumerate(ranges)]
    for load in loads:
        load.start()
    for load, at, store in zip(loads, ranges, stores):
        load.wait()
        wide[at, :] = narrow[at, :].astype(jnp.float32)
        store.start()
    for store in stores:
        store.wait()


def fused_body(spectra, bin_index):
    parts, segs, bins, stations = spectra.shape
    blocks = lax.axis_size("sta")
    depth = parts * segs * bins
    chunk = stations // 2
    quarter = chunk // 2
    scale = 1.0 / math.sqrt(segs * lax.axis_size("seg") * bins)
    tasks = 24
    low = jnp.bfloat16
    out = pl.pallas_call(
        functools.partial(kernel, (segs, bins, chunk, scale)),
        out_shape=jax.ShapeDtypeStruct((LAGS * quarter, blocks * stations), low),
        in_specs=[
            pl.BlockSpec(memory_space=pl.ANY),
            pl.BlockSpec(memory_space=pltpu.VMEM),
        ],
        out_specs=pl.BlockSpec(memory_space=pl.ANY),
        scratch_shapes=[
            pltpu.VMEM((12, depth, chunk), low),
            pltpu.VMEM((2, depth, chunk), low),
            pltpu.VMEM((4, 2, LAGS * chunk, depth), low),
            pltpu.VMEM((tasks, 2, 2, LAGS * quarter, chunk), low),
            pltpu.VMEM((tasks, 2, LAGS * quarter, chunk), low),
            pltpu.VMEM((tasks, LAGS * quarter, chunk), low),
            pltpu.VMEM((bins, bins), low),
            pltpu.VMEM((bins, chunk), jnp.float32),
            pltpu.VMEM((LAGS, bins), jnp.float32),
            pltpu.VMEM((LAGS, bins), jnp.float32),
            pltpu.SemaphoreType.DMA((2,)),
            pltpu.SemaphoreType.DMA((10, 2)),
            pltpu.SemaphoreType.DMA((15,)),
            pltpu.SemaphoreType.DMA((tasks,)),
            pltpu.SemaphoreType.DMA((tasks,)),
            pltpu.SemaphoreType.DMA((tasks,)),
            pltpu.SemaphoreType.DMA((tasks,)),
            pltpu.SemaphoreType.DMA((tasks,)),
            pltpu.SemaphoreType.DMA((14,)),
        ],
        compiler_params=pltpu.CompilerParams(
            collective_id=0, has_side_effects=True, vmem_limit_bytes=67_043_328
        ),
    )(spectra.reshape(depth, stations), bin_index.reshape(1, bins))
    steps = 8
    any_space = pl.BlockSpec(memory_space=pl.ANY)
    out = pl.pallas_call(
        functools.partial(widen, steps),
        out_shape=jax.ShapeDtypeStruct(out.shape, jnp.float32),
        in_specs=[any_space],
        out_specs=any_space,
        scratch_shapes=[
            pltpu.VMEM(out.shape, low),
            pltpu.VMEM(out.shape, jnp.float32),
            pltpu.SemaphoreType.DMA((steps,)),
            pltpu.SemaphoreType.DMA((steps,)),
        ],
    )(out)
    return out.reshape(LAGS, quarter, blocks * stations)


def solution(mesh):
    placed = (P(None, "seg", None, "sta"), P())
    chosen = fused_body if (mesh.shape["sta"], mesh.shape["seg"]) == (8, 4) else general_body
    return jax.shard_map(
        chosen, mesh=mesh, in_specs=placed, out_specs=P(None, ("sta", "seg"), None), check_vma=False
    )
```

```python
import functools
import math

import jax
import jax.numpy as jnp
from jax import lax
from jax.experimental import pallas as pl
from jax.experimental.pallas import tpu as pltpu
from jax.sharding import PartitionSpec as P

NFFT = 8192
LAGS = 2
LAG_STEP = 37
HALF = 64
MESH = pl.DeviceIdType.MESH


def whiten(spectra):
    values = spectra.astype(jnp.float32)
    energy = values[0] * values[0] + values[1] * values[1]
    freq_bins = values.shape[2]
    bin_pos = jnp.arange(freq_bins, dtype=jnp.int32)
    window = (jnp.abs(bin_pos[:, None] - bin_pos[None, :]) <= HALF).astype(jnp.float32)
    bin_count = jnp.sum(window, axis=1)
    smoothed = (
        jnp.einsum("gf,sfc->sgc", window, energy, precision=lax.Precision.HIGHEST)
        / bin_count[None, :, None]
    )
    return (values / jnp.sqrt(smoothed + 1e-06)[None]).astype(jnp.bfloat16)


def phases(bin_index):
    lag_samples = (jnp.arange(LAGS, dtype=jnp.int32) + 1) * LAG_STEP
    phase_turn = lag_samples[:, None] * bin_index[None, :] % NFFT
    phase_angle = 2.0 * math.pi / NFFT * phase_turn.astype(jnp.float32)
    return (jnp.cos(phase_angle), jnp.sin(phase_angle))


def rotate(whitened, cosine, sine_part):
    real_part = whitened[0].astype(jnp.float32)[None]
    imag_part = whitened[1].astype(jnp.float32)[None]
    cos_part = cosine[:, None, :, None]
    sin_part = sine_part[:, None, :, None]
    rot_real = real_part * cos_part - imag_part * sin_part
    rot_imag = real_part * sin_part + imag_part * cos_part
    stacked = jnp.stack([rot_real, rot_imag], axis=1).astype(jnp.bfloat16)
    return stacked.reshape(cosine.shape[0], -1, whitened.shape[3])


def pair_block(rotated, columns, norm_scale):
    product = jnp.einsum("mki,kj->mij", rotated, columns, preferred_element_type=jnp.float32)
    return (product * norm_scale).astype(jnp.bfloat16)


def general_body(spectra, bin_index):
    whitened = whiten(spectra)
    cosine, sine_part = phases(bin_index)
    seg_local = whitened.shape[1]
    freq_bins = whitened.shape[2]
    norm_scale = 1.0 / math.sqrt(seg_local * lax.axis_size("seg") * freq_bins)
    rotated = rotate(whitened, cosine, sine_part)
    shard_cols = lax.all_gather(whitened, "sta", axis=3, tiled=True)
    columns = shard_cols.reshape(-1, shard_cols.shape[3])
    product = pair_block(rotated, columns, norm_scale)
    return lax.psum_scatter(product, "seg", scatter_dimension=1, tiled=True).astype(jnp.float32)


OWN, SIDE, END, END_SIDE, MID, FAR = 0, 2, 4, 6, 8, 10


def kernel(
    dims, src, bin_ref, out, cols, raw_kept, rows, part, from_core, from_x, window, inv_count, cos_ref, sin_ref,
    load_sem, send_sem, recv_sem, core_send, core_recv, x_send, x_recv, out_send, out_recv,
):
    segs, bins, chunk, scale = dims
    depth = 2 * segs * bins
    half = segs * bins
    quarter = chunk // 2
    sta = lax.axis_index("sta")
    seg = lax.axis_index("seg")
    z, y = sta // 2, sta % 2
    x, core = seg // 2, seg % 2
    z_near = z + 1 - 2 * (z % 2)
    is_mid = ((z + 1) // 2) % 2
    side = z * 2 + (1 - y)
    near = z_near * 2 + y
    near_side = z_near * 2 + (1 - y)
    mid = (3 - z) * 2 + y
    far = ((z + 2) % 4) * 2 + y
    core_seg = x * 2 + (1 - core)
    x_seg = (1 - x) * 2 + core

    barrier = pltpu.get_barrier_semaphore()
    for partner in ((sta, core_seg), (sta, x_seg), (side, seg), (near, seg), (near_side, seg)):
        pl.semaphore_signal(barrier, inc=1, device_id=partner, device_id_type=MESH)

    @pl.when(is_mid == 1)
    def _():
        pl.semaphore_signal(barrier, inc=1, device_id=(mid, seg), device_id_type=MESH)

    loads = [
        pltpu.make_async_copy(
            src.at[:, pl.ds(ch * chunk, chunk)], cols.at[OWN + ch], load_sem.at[ch]
        )
        for ch in range(2)
    ]
    for load in loads:
        load.start()
    pl.semaphore_wait(barrier, 5 + is_mid)

    def remote(source, target, send, recv, to_sta, to_seg):
        return pltpu.make_async_remote_copy(
            src_ref=source, dst_ref=target, send_sem=send, recv_sem=recv,
            device_id=(to_sta, to_seg), device_id_type=MESH,
        )

    def own_chunk(ch):
        return src.at[:, pl.ds(ch * chunk, chunk)]

    def landing(slot, ends):
        kept = SIDE if ends else END
        return raw_kept.at[slot - kept] if kept <= slot < kept + 2 else cols.at[slot]

    def push(source, target, slot, index, to_sta):
        copy = remote(source, target, send_sem.at[index, 0], recv_sem.at[slot], to_sta, seg)
        copy.start()
        return copy

    second = {FAR + 1: 12, END_SIDE: 13, END_SIDE + 1: 14}

    def push_pieces(sends, source, slot, index, to_sta):
        for piece in range(2):
            lanes = pl.ds(piece * quarter, quarter)
            copy = remote(
                source.at[:, lanes], cols.at[slot, :, lanes],
                send_sem.at[index, piece], recv_sem.at[second[slot] if piece else slot], to_sta, seg,
            )
            copy.start()
            sends.append(copy)

    def piece_arrived(slot, piece):
        there = cols.at[slot, :, pl.ds(piece * quarter, quarter)]
        remote(
            there, there, send_sem.at[0, 0], recv_sem.at[second[slot] if piece else slot], side, seg
        ).wait_recv()

    def arrived(slot, ends):
        there = landing(slot, ends)
        remote(there, there, send_sem.at[0, 0], recv_sem.at[slot], side, seg).wait_recv()


    row_at = lax.broadcasted_iota(jnp.int32, (bins, bins), 0)
    col_at = lax.broadcasted_iota(jnp.int32, (bins, bins), 1)
    band = jnp.where(jnp.abs(row_at - col_at) <= HALF, 1.0, 0.0).astype(jnp.bfloat16)
    window[...] = band
    pos = lax.broadcasted_iota(jnp.int32, (bins, chunk), 0)
    count = jnp.minimum(pos, HALF) + jnp.minimum(bins - 1 - pos, HALF) + 1
    inv_count[...] = 1.0 / count.astype(jnp.float32)

    for lag in range(LAGS):
        turn = lax.rem((lag + 1) * LAG_STEP * bin_ref[...], NFFT)
        angle = 2.0 * math.pi / NFFT * turn.astype(jnp.float32)
        cos_ref[lag : lag + 1, :] = jnp.cos(angle)
        sin_ref[lag : lag + 1, :] = jnp.sin(angle)

    def whiten_lanes(slot, ends, first, width):
        raw = landing(slot, ends)
        lanes = pl.ds(first, width)

        def one(s, carry):
            at_re = pl.ds(pl.multiple_of(s * bins, bins), bins)
            at_im = pl.ds(pl.multiple_of(half + s * bins, bins), bins)
            real = raw[at_re, lanes].astype(jnp.float32)
            imag = raw[at_im, lanes].astype(jnp.float32)
            energy = real * real + imag * imag
            total = jnp.dot(window[...], energy.astype(jnp.bfloat16), preferred_element_type=jnp.float32)
            gain = lax.rsqrt(total * inv_count[:, :width] + 1e-06)
            real = raw[at_re, lanes].astype(jnp.float32)
            imag = raw[at_im, lanes].astype(jnp.float32)
            cols[slot, at_re, lanes] = (real * gain).astype(jnp.bfloat16)
            cols[slot, at_im, lanes] = (imag * gain).astype(jnp.bfloat16)
            return carry

        lax.fori_loop(0, segs, one, 0)

    def whiten_chunk(slot, ends):
        whiten_lanes(slot, ends, 0, chunk)

    def rotate_chunk(row, slot, first=0, pieces=2):
        xq = slot % 2

        def one(step, carry):
            parity, s = first + step // segs, step % segs
            lanes = pl.ds(pl.multiple_of(parity * quarter, quarter), quarter)
            at_re = pl.ds(pl.multiple_of(s * bins, bins), bins)
            at_im = pl.ds(pl.multiple_of(half + s * bins, bins), bins)
            real = cols[slot, at_re, lanes].T.astype(jnp.float32)
            imag = cols[slot, at_im, lanes].T.astype(jnp.float32)
            for lag in range(LAGS):
                cosine = cos_ref[lag : lag + 1, :]
                sine = sin_ref[lag : lag + 1, :]
                at = pl.ds(xq * LAGS * quarter + lag * quarter, quarter)
                rows[row, parity, at, at_re] = (real * cosine - imag * sine).astype(jnp.bfloat16)
                rows[row, parity, at, at_im] = (real * sine + imag * cosine).astype(jnp.bfloat16)
            return carry

        lax.fori_loop(0, pieces * segs, one, 0)

    away = {}
    guests = {FAR: 14, MID + 1: 15}

    def away_copy(task):
        index, slot = task[0], task[2]
        return remote(
            part.at[index, 1], part.at[away[index], 1], out_send.at[index], out_recv.at[slot - 4], near_side, seg
        )

    def core_copy(task):
        index, width = task[0], task[4]
        return remote(
            part.at[index, 0, :, :, pl.ds(0, width)], from_core.at[index, :, :, pl.ds(0, width)],
            core_send.at[index], core_recv.at[index], sta, core_seg,
        )

    def x_copy(task):
        index, width = task[0], task[4]
        return remote(
            part.at[index, 1, 1 - x, :, pl.ds(0, width)], from_x.at[index, :, pl.ds(0, width)],
            x_send.at[index], x_recv.at[index], sta, x_seg,
        )

    def lanes_at(task, ends):
        index, row, slot, first, width = task
        if ends:
            station = {OWN: sta, SIDE: side, MID: near, FAR: far}[slot - slot % 2]
        else:
            station = {OWN: sta, SIDE: side, MID: mid, FAR: far}[slot - slot % 2]
        if ends and index in guests.values():
            station = (((z + 2) % 4) if slot == MID + 1 else 3 - z) * 2 + (1 - y)
        start = (station * 4 + (slot % 2) * 2 + first // quarter) * quarter
        return pl.ds(pl.multiple_of(start, quarter), width)

    def out_copy(task, ends):
        index, row, slot, first, width = task
        source = part.at[index, 1, x, :, pl.ds(0, width)]
        target = out.at[:, lanes_at(task, ends)]
        to_sta = {1: side, 2: near, 3: near_side}[row]
        if first > 0:
            arrival = 13 if row == 3 else 12
        elif row == 3:
            arrival = slot - 4
        elif row == 1 and ends:
            arrival = slot - MID
        else:
            arrival = slot
        return remote(source, target, out_send.at[index], out_recv.at[arrival], to_sta, seg)

    def compute(task):
        index, row, slot, first, width = task

        def one(h, carry):
            parity = (core + 1 + h) % 2
            product = jnp.dot(
                rows[row, parity], cols[slot, :, pl.ds(first, width)], preferred_element_type=jnp.float32
            )
            product = (product * scale).astype(jnp.bfloat16)
            part[index, h, 0, :, :width] = product[: LAGS * quarter]
            part[index, h, 1, :, :width] = product[LAGS * quarter :]

            @pl.when(h == 0)
            def _():
                core_copy(task).start()

            return carry

        lax.fori_loop(0, 2, one, 0)

    def add_into(index, xq, other, width):
        def one(step, carry):
            at = pl.ds(pl.multiple_of(step * 64, 64), 64)
            mine = part[index, 1, xq, at, :width].astype(jnp.float32)
            part[index, 1, xq, at, :width] = (mine + other[at, :width].astype(jnp.float32)).astype(jnp.bfloat16)
            return carry

        lax.fori_loop(0, LAGS * quarter // 64, one, 0)

    def finish_core(task):
        index, width = task[0], task[4]
        core_copy(task).wait_recv()
        add_into(index, 1 - x, from_core.at[index, 1 - x], width)
        if index not in away:
            x_copy(task).start()
        add_into(index, x, from_core.at[index, x], width)
        if index in away:
            away_copy(task).start()

    def finish_x(task, ends):
        index, width = task[0], task[4]
        if index in away:
            return
        x_copy(task).wait_recv()
        if task[1] > 0:
            add_into(index, x, from_x.at[index], width)
            out_copy(task, ends).start()
            return
        lanes = lanes_at(task, ends)

        def one(step, carry):
            at = pl.ds(pl.multiple_of(step * 64, 64), 64)
            mine = part[index, 1, x, at, :width].astype(jnp.float32)
            out[at, lanes] = (mine + from_x[index, at, :width].astype(jnp.float32)).astype(jnp.bfloat16)
            return carry

        lax.fori_loop(0, LAGS * quarter // 64, one, 0)

    class Flow:
        def __init__(self, ends):
            self.ends = ends
            self.done = []
            self.at_core = 0
            self.at_x = 0

        def task(self, row, slot, first=0, width=chunk, core_lag=1, x_lag=3):
            self.done.append((len(self.done), row, slot, first, width))
            compute(self.done[-1])
            self.advance(core_lag, x_lag)

        def advance(self, core_lag, x_lag):
            while self.at_core < len(self.done) - core_lag:
                finish_core(self.done[self.at_core])
                self.at_core += 1
            while self.at_x < len(self.done) - x_lag:
                finish_x(self.done[self.at_x], self.ends)
                self.at_x += 1

        def drain(self):
            self.advance(0, 0)
            for task in self.done:
                core_copy(task).wait_send()
                if task[0] in away:
                    away_copy(task).wait_send()
                    continue
                x_copy(task).wait_send()
                if task[1] > 0:
                    out_copy(task, self.ends).wait_send()

    def incoming(index, width):
        target = out.at[:, pl.ds(0, width)]
        remote(target, target, out_send.at[0], out_recv.at[index], side, seg).wait_recv()

    def start_own(flow):
        for ch in range(2):
            loads[ch].wait()
            whiten_chunk(OWN + ch, flow.ends)
            rotate_chunk(0, OWN + ch)
        for ch in range(2):
            flow.task(0, OWN + ch)
        flow.advance(0, 0)

    def leave(flow, sends, expected):
        flow.drain()
        for copy in sends:
            copy.wait_send()
        for index, width in expected:
            incoming(index, width)

    @pl.when(is_mid == 0)
    def _():
        sends = []
        for ch in range(2):
            sends.append(push(own_chunk(ch), raw_kept.at[ch], END + ch, 2 + ch, near))
            sends.append(push(own_chunk(ch), raw_kept.at[ch], SIDE + ch, ch, side))
        flow = Flow(True)
        start_own(flow)
        for ch in range(2):
            arrived(SIDE + ch, True)
            if ch == 0:
                push_pieces(sends, raw_kept.at[0], END_SIDE, 4, near)
            whiten_chunk(SIDE + ch, True)
            rotate_chunk(1, SIDE + ch)
            flow.task(0, SIDE + ch)
            arrived(MID + ch, True)
            whiten_chunk(MID + ch, True)
            rotate_chunk(2, MID + ch)
            flow.task(0, MID + ch)
            if ch == 0:
                flow.advance(0, 0)
        for row, slot in ((2, OWN), (2, OWN + 1), (2, SIDE), (2, SIDE + 1), (1, MID), (1, MID + 1)):
            flow.task(row, slot)
        arrived(FAR, True)
        flow.task(1, FAR)
        flow.task(0, FAR)
        flow.advance(0, 0)
        stays = []
        for slot in (FAR, MID + 1):
            index = guests[slot]
            there = part.at[index, 1]
            remote(there, there, send_sem.at[0, 0], out_recv.at[slot - 4], near_side, seg).wait_recv()
            stays.append((index, 0, slot, 0, chunk))
            x_copy(stays[-1]).start()
        for task in stays:
            finish_x(task, True)
        for task in stays:
            x_copy(task).wait_send()
        expected = [(index, chunk) for index in (0, 1, 2, 9, 10)]
        expected += [(7, quarter), (11, quarter), (12, quarter), (13, quarter)]
        leave(flow, sends, expected)

    @pl.when(is_mid == 1)
    def _():
        sends = []
        for ch in range(2):
            sends.append(push(own_chunk(ch), cols.at[MID + ch], MID + ch, 2 + ch, mid))
            sends.append(push(own_chunk(ch), cols.at[SIDE + ch], SIDE + ch, ch, side))
            sends.append(push(own_chunk(ch), cols.at[MID + ch], MID + ch, 8 + ch, near))

        def relay(slot):
            arrived(slot, False)
            if slot == END:
                sends.append(push(raw_kept.at[0], cols.at[FAR], FAR, 4, mid))
                return
            push_pieces(sends, raw_kept.at[1], FAR + 1, 5, mid)
            push_pieces(sends, raw_kept.at[1], END_SIDE + 1, 7, side)

        def ready(slot, row=None):
            if not END <= slot < END + 2:
                arrived(slot, False)
            whiten_chunk(slot, False)
            if row is not None:
                rotate_chunk(row, slot)

        def ready_piece(slot, piece, row=None):
            piece_arrived(slot, piece)
            whiten_lanes(slot, False, piece * quarter, quarter)
            if row is not None:
                rotate_chunk(row, slot, piece, 1)

        flow = Flow(False)
        start_own(flow)
        relay(END)
        ready(SIDE, 1)
        flow.task(0, SIDE)
        ready(MID)
        flow.task(0, MID)
        sends.append(push(cols.at[MID], cols.at[FAR], FAR, 9, near))
        ready(END, 2)
        flow.advance(0, 0)
        relay(END + 1)
        ready(MID + 1)
        flow.task(0, MID + 1)
        ready(END + 1, 2)
        flow.task(2, MID + 1)
        ready(SIDE + 1, 1)
        for row, slot in ((1, MID), (1, MID + 1), (0, SIDE + 1)):
            flow.task(row, slot, x_lag=6)
        flow.advance(0, 3)
        for ch in range(2):
            ready_piece(END_SIDE + ch, 0, 3)
        ready(FAR)
        for row in (2, 1, 0):
            flow.task(row, FAR, x_lag=6)
        for ch in range(2):
            ready_piece(END_SIDE + ch, 1, 3)
        for slot in (FAR, MID + 1):
            away[len(flow.done)] = guests[slot]
            flow.task(3, slot, x_lag=6)
        for piece in range(2):
            first = piece * quarter
            ready_piece(FAR + 1, piece)
            for row in (3, 2, 1, 0):
                flow.task(row, FAR + 1, first, quarter, x_lag=6 - 2 * piece)
            if piece == 0:
                flow.advance(0, 4)
        flow.advance(1, 3)
        expected = [(index, chunk) for index in (0, 1, 2, 3, 8, 9, 10)] + [(11, quarter), (12, quarter)]
        leave(flow, sends, expected)


def widen(steps, src, out, wide, out_sem):
    rows = src.shape[0] // steps
    ranges = [pl.ds(step * rows, rows) for step in range(steps)]
    stores = [pltpu.make_async_copy(wide.at[at], out.at[at], out_sem.at[i]) for i, at in enumerate(ranges)]
    for at, store in zip(ranges, stores):
        wide[at, :] = src[at, :].astype(jnp.float32)
        store.start()
    for store in stores:
        store.wait()


def fused_body(spectra, bin_index):
    parts, segs, bins, stations = spectra.shape
    blocks = lax.axis_size("sta")
    depth = parts * segs * bins
    chunk = stations // 2
    quarter = chunk // 2
    scale = 1.0 / math.sqrt(segs * lax.axis_size("seg") * bins)
    tasks = 24
    low = jnp.bfloat16
    out = pl.pallas_call(
        functools.partial(kernel, (segs, bins, chunk, scale)),
        out_shape=pltpu.VMEM((LAGS * quarter, blocks * stations), low),
        in_specs=[
            pl.BlockSpec(memory_space=pl.ANY),
            pl.BlockSpec(memory_space=pltpu.VMEM),
        ],
        out_specs=pl.BlockSpec(memory_space=pltpu.VMEM),
        scratch_shapes=[
            pltpu.VMEM((12, depth, chunk), low),
            pltpu.VMEM((2, depth, chunk), low),
            pltpu.VMEM((4, 2, LAGS * chunk, depth), low),
            pltpu.VMEM((tasks, 2, 2, LAGS * quarter, chunk), low),
            pltpu.VMEM((tasks, 2, LAGS * quarter, chunk), low),
            pltpu.VMEM((tasks, LAGS * quarter, chunk), low),
            pltpu.VMEM((bins, bins), low),
            pltpu.VMEM((bins, chunk), jnp.float32),
            pltpu.VMEM((LAGS, bins), jnp.float32),
            pltpu.VMEM((LAGS, bins), jnp.float32),
            pltpu.SemaphoreType.DMA((2,)),
            pltpu.SemaphoreType.DMA((10, 2)),
            pltpu.SemaphoreType.DMA((15,)),
            pltpu.SemaphoreType.DMA((tasks,)),
            pltpu.SemaphoreType.DMA((tasks,)),
            pltpu.SemaphoreType.DMA((tasks,)),
            pltpu.SemaphoreType.DMA((tasks,)),
            pltpu.SemaphoreType.DMA((tasks,)),
            pltpu.SemaphoreType.DMA((14,)),
        ],
        compiler_params=pltpu.CompilerParams(
            collective_id=0, has_side_effects=True, vmem_limit_bytes=58 * 1024 * 1024
        ),
    )(spectra.reshape(depth, stations), bin_index.reshape(1, bins))
    return out.reshape(LAGS, quarter, blocks * stations).astype(jnp.float32)


def solution(mesh):
    placed = (P(None, "seg", None, "sta"), P())
    chosen = fused_body if (mesh.shape["sta"], mesh.shape["seg"]) == (8, 4) else general_body
    return jax.shard_map(
        chosen, mesh=mesh, in_specs=placed, out_specs=P(None, ("sta", "seg"), None), check_vma=False
    )
```

```python
import functools
import math

import jax
import jax.numpy as jnp
from jax import lax
from jax.experimental import pallas as pl
from jax.experimental.pallas import tpu as pltpu
from jax.sharding import PartitionSpec as P

NFFT = 8192
LAGS = 2
LAG_STEP = 37
HALF = 64
MESH = pl.DeviceIdType.MESH


def whiten(spectra):
    values = spectra.astype(jnp.float32)
    energy = values[0] * values[0] + values[1] * values[1]
    freq_bins = values.shape[2]
    bin_pos = jnp.arange(freq_bins, dtype=jnp.int32)
    window = (jnp.abs(bin_pos[:, None] - bin_pos[None, :]) <= HALF).astype(jnp.float32)
    bin_count = jnp.sum(window, axis=1)
    smoothed = (
        jnp.einsum("gf,sfc->sgc", window, energy, precision=lax.Precision.HIGHEST)
        / bin_count[None, :, None]
    )
    return (values / jnp.sqrt(smoothed + 1e-06)[None]).astype(jnp.bfloat16)


def phases(bin_index):
    lag_samples = (jnp.arange(LAGS, dtype=jnp.int32) + 1) * LAG_STEP
    phase_turn = lag_samples[:, None] * bin_index[None, :] % NFFT
    phase_angle = 2.0 * math.pi / NFFT * phase_turn.astype(jnp.float32)
    return (jnp.cos(phase_angle), jnp.sin(phase_angle))


def rotate(whitened, cosine, sine_part):
    real_part = whitened[0].astype(jnp.float32)[None]
    imag_part = whitened[1].astype(jnp.float32)[None]
    cos_part = cosine[:, None, :, None]
    sin_part = sine_part[:, None, :, None]
    rot_real = real_part * cos_part - imag_part * sin_part
    rot_imag = real_part * sin_part + imag_part * cos_part
    stacked = jnp.stack([rot_real, rot_imag], axis=1).astype(jnp.bfloat16)
    return stacked.reshape(cosine.shape[0], -1, whitened.shape[3])


def pair_block(rotated, columns, norm_scale):
    product = jnp.einsum("mki,kj->mij", rotated, columns, preferred_element_type=jnp.float32)
    return (product * norm_scale).astype(jnp.bfloat16)


def general_body(spectra, bin_index):
    whitened = whiten(spectra)
    cosine, sine_part = phases(bin_index)
    seg_local = whitened.shape[1]
    freq_bins = whitened.shape[2]
    norm_scale = 1.0 / math.sqrt(seg_local * lax.axis_size("seg") * freq_bins)
    rotated = rotate(whitened, cosine, sine_part)
    shard_cols = lax.all_gather(whitened, "sta", axis=3, tiled=True)
    columns = shard_cols.reshape(-1, shard_cols.shape[3])
    product = pair_block(rotated, columns, norm_scale)
    return lax.psum_scatter(product, "seg", scatter_dimension=1, tiled=True).astype(jnp.float32)


OWN, SIDE, END, END_SIDE, MID, FAR = 0, 2, 4, 6, 8, 10


def kernel(
    dims, src, bin_ref, out, cols, raw_kept, rows, part, from_core, from_x, window, inv_count, begun, cos_ref, sin_ref,
    load_sem, send_sem, recv_sem, core_send, core_recv, x_send, x_recv, out_send, out_recv,
):
    segs, bins, chunk, scale = dims
    depth = 2 * segs * bins
    half = segs * bins
    quarter = chunk // 2
    sta = lax.axis_index("sta")
    seg = lax.axis_index("seg")
    z, y = sta // 2, sta % 2
    x, core = seg // 2, seg % 2
    z_near = z + 1 - 2 * (z % 2)
    is_mid = ((z + 1) // 2) % 2
    side = z * 2 + (1 - y)
    near = z_near * 2 + y
    near_side = z_near * 2 + (1 - y)
    mid = (3 - z) * 2 + y
    far = ((z + 2) % 4) * 2 + y
    core_seg = x * 2 + (1 - core)
    x_seg = (1 - x) * 2 + core

    barrier = pltpu.get_barrier_semaphore()
    for partner in ((sta, core_seg), (sta, x_seg), (side, seg), (near, seg), (near_side, seg)):
        pl.semaphore_signal(barrier, inc=1, device_id=partner, device_id_type=MESH)

    @pl.when(is_mid == 1)
    def _():
        pl.semaphore_signal(barrier, inc=1, device_id=(mid, seg), device_id_type=MESH)

    loads = [
        pltpu.make_async_copy(
            src.at[:, pl.ds(ch * chunk, chunk)], cols.at[OWN + ch], load_sem.at[ch]
        )
        for ch in range(2)
    ]
    for load in loads:
        load.start()
    pl.semaphore_wait(barrier, 5 + is_mid)

    def remote(source, target, send, recv, to_sta, to_seg):
        return pltpu.make_async_remote_copy(
            src_ref=source, dst_ref=target, send_sem=send, recv_sem=recv,
            device_id=(to_sta, to_seg), device_id_type=MESH,
        )

    def own_chunk(ch):
        return src.at[:, pl.ds(ch * chunk, chunk)]

    def landing(slot, ends):
        kept = SIDE if ends else END
        return raw_kept.at[slot - kept] if kept <= slot < kept + 2 else cols.at[slot]

    def push(source, target, slot, index, to_sta):
        copy = remote(source, target, send_sem.at[index, 0], recv_sem.at[slot], to_sta, seg)
        copy.start()
        return copy

    second = {FAR + 1: 12, END_SIDE: 13, END_SIDE + 1: 14}

    def segment_copy(source, s, wave, to_sta):
        at = (pl.ds(wave * half + s * bins, bins), pl.ds(quarter, quarter))
        return remote(
            source.at[at], cols.at[FAR + 1].at[at],
            send_sem.at[10 + 2 * s + wave, 0], recv_sem.at[15 + 2 * s + wave], to_sta, seg,
        )

    def push_pieces(sends, source, slot, index, to_sta):
        for piece in range(2):
            lanes = pl.ds(piece * quarter, quarter)
            if slot == FAR + 1 and piece == 1:
                for s in range(segs):
                    for wave in range(2):
                        copy = segment_copy(source, s, wave, to_sta)
                        copy.start()
                        sends.append(copy)
                continue
            copy = remote(
                source.at[:, lanes], cols.at[slot, :, lanes],
                send_sem.at[index, piece], recv_sem.at[second[slot] if piece else slot], to_sta, seg,
            )
            copy.start()
            sends.append(copy)

    def piece_arrived(slot, piece):
        there = cols.at[slot, :, pl.ds(piece * quarter, quarter)]
        remote(
            there, there, send_sem.at[0, 0], recv_sem.at[second[slot] if piece else slot], side, seg
        ).wait_recv()

    def arrived(slot, ends):
        there = landing(slot, ends)
        remote(there, there, send_sem.at[0, 0], recv_sem.at[slot], side, seg).wait_recv()


    row_at = lax.broadcasted_iota(jnp.int32, (bins, bins), 0)
    col_at = lax.broadcasted_iota(jnp.int32, (bins, bins), 1)
    band = jnp.where(jnp.abs(row_at - col_at) <= HALF, 1.0, 0.0).astype(jnp.bfloat16)
    window[...] = band
    pos = lax.broadcasted_iota(jnp.int32, (bins, chunk), 0)
    count = jnp.minimum(pos, HALF) + jnp.minimum(bins - 1 - pos, HALF) + 1
    inv_count[...] = 1.0 / count.astype(jnp.float32)

    for lag in range(LAGS):
        turn = lax.rem((lag + 1) * LAG_STEP * bin_ref[...], NFFT)
        angle = 2.0 * math.pi / NFFT * turn.astype(jnp.float32)
        cos_ref[lag : lag + 1, :] = jnp.cos(angle)
        sin_ref[lag : lag + 1, :] = jnp.sin(angle)

    def rows_of(wave, s):
        start = wave * half + s * bins
        return pl.ds(start if isinstance(start, int) else pl.multiple_of(start, bins), bins)

    def whiten_lanes(slot, ends, first, width, only=None):
        raw = landing(slot, ends)
        lanes = pl.ds(first, width)

        def one(s, carry):
            at_re = rows_of(0, s)
            at_im = rows_of(1, s)
            real = raw[at_re, lanes].astype(jnp.float32)
            imag = raw[at_im, lanes].astype(jnp.float32)
            energy = real * real + imag * imag
            total = jnp.dot(window[...], energy.astype(jnp.bfloat16), preferred_element_type=jnp.float32)
            gain = lax.rsqrt(total * inv_count[:, :width] + 1e-06)
            real = raw[at_re, lanes].astype(jnp.float32)
            imag = raw[at_im, lanes].astype(jnp.float32)
            cols[slot, at_re, lanes] = (real * gain).astype(jnp.bfloat16)
            cols[slot, at_im, lanes] = (imag * gain).astype(jnp.bfloat16)
            return carry

        if only is None:
            lax.fori_loop(0, segs, one, 0)
        else:
            one(only, 0)

    def whiten_chunk(slot, ends):
        whiten_lanes(slot, ends, 0, chunk)

    def rotate_chunk(row, slot, first=0, pieces=2):
        xq = slot % 2

        def one(step, carry):
            parity, s = first + step // segs, step % segs
            lanes = pl.ds(pl.multiple_of(parity * quarter, quarter), quarter)
            at_re = pl.ds(pl.multiple_of(s * bins, bins), bins)
            at_im = pl.ds(pl.multiple_of(half + s * bins, bins), bins)
            real = cols[slot, at_re, lanes].T.astype(jnp.float32)
            imag = cols[slot, at_im, lanes].T.astype(jnp.float32)
            for lag in range(LAGS):
                cosine = cos_ref[lag : lag + 1, :]
                sine = sin_ref[lag : lag + 1, :]
                at = pl.ds(xq * LAGS * quarter + lag * quarter, quarter)
                rows[row, parity, at, at_re] = (real * cosine - imag * sine).astype(jnp.bfloat16)
                rows[row, parity, at, at_im] = (real * sine + imag * cosine).astype(jnp.bfloat16)
            return carry

        lax.fori_loop(0, pieces * segs, one, 0)

    away = {}
    guests = {FAR: 14, MID + 1: 15}

    def away_copy(task):
        index, slot = task[0], task[2]
        return remote(
            part.at[index, 1], part.at[away[index], 1], out_send.at[index], out_recv.at[slot - 4], near_side, seg
        )

    def core_copy(task):
        index, width = task[0], task[4]
        return remote(
            part.at[index, 0, :, :, pl.ds(0, width)], from_core.at[index, :, :, pl.ds(0, width)],
            core_send.at[index], core_recv.at[index], sta, core_seg,
        )

    def x_copy(task):
        index, width = task[0], task[4]
        return remote(
            part.at[index, 1, 1 - x, :, pl.ds(0, width)], from_x.at[index, :, pl.ds(0, width)],
            x_send.at[index], x_recv.at[index], sta, x_seg,
        )

    def lanes_at(task, ends):
        index, row, slot, first, width = task
        if ends:
            station = {OWN: sta, SIDE: side, MID: near, FAR: far}[slot - slot % 2]
        else:
            station = {OWN: sta, SIDE: side, MID: mid, FAR: far}[slot - slot % 2]
        if ends and index in guests.values():
            station = (((z + 2) % 4) if slot == MID + 1 else 3 - z) * 2 + (1 - y)
        start = (station * 4 + (slot % 2) * 2 + first // quarter) * quarter
        return pl.ds(pl.multiple_of(start, quarter), width)

    def out_copy(task, ends):
        index, row, slot, first, width = task
        source = part.at[index, 1, x, :, pl.ds(0, width)]
        target = out.at[:, lanes_at(task, ends)]
        to_sta = {1: side, 2: near, 3: near_side}[row]
        if first > 0:
            arrival = 13 if row == 3 else 12
        elif row == 3:
            arrival = slot - 4
        elif row == 1 and ends:
            arrival = slot - MID
        else:
            arrival = slot
        return remote(source, target, out_send.at[index], out_recv.at[arrival], to_sta, seg)

    def dot_segment(row, parity, slot, lanes, s):
        return sum(
            jnp.dot(
                rows[row, parity, :, rows_of(wave, s)], cols[slot, rows_of(wave, s), lanes],
                preferred_element_type=jnp.float32,
            )
            for wave in range(2)
        )

    def begin(row, slot, first, width, s):
        def one(h, carry):
            product = dot_segment(row, (core + 1 + h) % 2, slot, pl.ds(first, width), s)
            begun[row, h] = product if s == 0 else begun[row, h] + product
            return carry

        lax.fori_loop(0, 2, one, 0)

    def compute(task, last):
        index, row, slot, first, width = task
        lanes = pl.ds(first, width)

        def one(h, carry):
            parity = (core + 1 + h) % 2
            if last is None:
                product = jnp.dot(rows[row, parity], cols[slot, :, lanes], preferred_element_type=jnp.float32)
            else:
                product = dot_segment(row, parity, slot, lanes, last)
                if last > 0:
                    product = begun[row, h] + product
            product = (product * scale).astype(jnp.bfloat16)
            part[index, h, 0, :, :width] = product[: LAGS * quarter]
            part[index, h, 1, :, :width] = product[LAGS * quarter :]

            @pl.when(h == 0)
            def _():
                core_copy(task).start()

            return carry

        lax.fori_loop(0, 2, one, 0)

    def add_into(index, xq, other, width):
        def one(step, carry):
            at = pl.ds(pl.multiple_of(step * 64, 64), 64)
            mine = part[index, 1, xq, at, :width].astype(jnp.float32)
            part[index, 1, xq, at, :width] = (mine + other[at, :width].astype(jnp.float32)).astype(jnp.bfloat16)
            return carry

        lax.fori_loop(0, LAGS * quarter // 64, one, 0)

    def finish_core(task):
        index, width = task[0], task[4]
        core_copy(task).wait_recv()
        add_into(index, 1 - x, from_core.at[index, 1 - x], width)
        if index not in away:
            x_copy(task).start()
        add_into(index, x, from_core.at[index, x], width)
        if index in away:
            away_copy(task).start()

    def finish_x(task, ends):
        index, width = task[0], task[4]
        if index in away:
            return
        x_copy(task).wait_recv()
        if task[1] > 0:
            add_into(index, x, from_x.at[index], width)
            out_copy(task, ends).start()
            return
        lanes = lanes_at(task, ends)

        def one(step, carry):
            at = pl.ds(pl.multiple_of(step * 64, 64), 64)
            mine = part[index, 1, x, at, :width].astype(jnp.float32)
            out[at, lanes] = (mine + from_x[index, at, :width].astype(jnp.float32)).astype(jnp.bfloat16)
            return carry

        lax.fori_loop(0, LAGS * quarter // 64, one, 0)

    class Flow:
        def __init__(self, ends):
            self.ends = ends
            self.done = []
            self.at_core = 0
            self.at_x = 0

        def task(self, row, slot, first=0, width=chunk, core_lag=1, x_lag=3, last=None):
            self.done.append((len(self.done), row, slot, first, width))
            compute(self.done[-1], last)
            self.advance(core_lag, x_lag)

        def advance(self, core_lag, x_lag):
            while self.at_core < len(self.done) - core_lag:
                finish_core(self.done[self.at_core])
                self.at_core += 1
            while self.at_x < len(self.done) - x_lag:
                finish_x(self.done[self.at_x], self.ends)
                self.at_x += 1

        def drain(self):
            self.advance(0, 0)
            for task in self.done:
                core_copy(task).wait_send()
                if task[0] in away:
                    away_copy(task).wait_send()
                    continue
                x_copy(task).wait_send()
                if task[1] > 0:
                    out_copy(task, self.ends).wait_send()

    def incoming(index, width):
        target = out.at[:, pl.ds(0, width)]
        remote(target, target, out_send.at[0], out_recv.at[index], side, seg).wait_recv()

    def start_own(flow):
        for ch in range(2):
            loads[ch].wait()
            whiten_chunk(OWN + ch, flow.ends)
            rotate_chunk(0, OWN + ch)
        for ch in range(2):
            flow.task(0, OWN + ch)
        flow.advance(0, 0)

    def leave(flow, sends, expected):
        flow.drain()
        for copy in sends:
            copy.wait_send()
        for index, width in expected:
            incoming(index, width)

    @pl.when(is_mid == 0)
    def _():
        sends = []
        for ch in range(2):
            sends.append(push(own_chunk(ch), raw_kept.at[ch], END + ch, 2 + ch, near))
            sends.append(push(own_chunk(ch), raw_kept.at[ch], SIDE + ch, ch, side))
        flow = Flow(True)
        start_own(flow)
        for ch in range(2):
            arrived(SIDE + ch, True)
            if ch == 0:
                push_pieces(sends, raw_kept.at[0], END_SIDE, 4, near)
            whiten_chunk(SIDE + ch, True)
            rotate_chunk(1, SIDE + ch)
            flow.task(0, SIDE + ch)
            arrived(MID + ch, True)
            whiten_chunk(MID + ch, True)
            rotate_chunk(2, MID + ch)
            flow.task(0, MID + ch)
            if ch == 0:
                flow.advance(0, 0)
        for row, slot in ((2, OWN), (2, OWN + 1), (2, SIDE), (2, SIDE + 1), (1, MID), (1, MID + 1)):
            flow.task(row, slot)
        arrived(FAR, True)
        flow.task(1, FAR)
        flow.task(0, FAR)
        flow.advance(0, 0)
        stays = []
        for slot in (FAR, MID + 1):
            index = guests[slot]
            there = part.at[index, 1]
            remote(there, there, send_sem.at[0, 0], out_recv.at[slot - 4], near_side, seg).wait_recv()
            stays.append((index, 0, slot, 0, chunk))
            x_copy(stays[-1]).start()
        for task in stays:
            finish_x(task, True)
        for task in stays:
            x_copy(task).wait_send()
        expected = [(index, chunk) for index in (0, 1, 2, 9, 10)]
        expected += [(7, quarter), (11, quarter), (12, quarter), (13, quarter)]
        leave(flow, sends, expected)

    @pl.when(is_mid == 1)
    def _():
        sends = []
        for ch in range(2):
            sends.append(push(own_chunk(ch), cols.at[MID + ch], MID + ch, 2 + ch, mid))
            sends.append(push(own_chunk(ch), cols.at[SIDE + ch], SIDE + ch, ch, side))
            sends.append(push(own_chunk(ch), cols.at[MID + ch], MID + ch, 8 + ch, near))

        def relay(slot):
            arrived(slot, False)
            if slot == END:
                sends.append(push(raw_kept.at[0], cols.at[FAR], FAR, 4, mid))
                return
            push_pieces(sends, raw_kept.at[1], FAR + 1, 5, mid)
            push_pieces(sends, raw_kept.at[1], END_SIDE + 1, 7, side)

        def ready(slot, row=None):
            if not END <= slot < END + 2:
                arrived(slot, False)
            whiten_chunk(slot, False)
            if row is not None:
                rotate_chunk(row, slot)

        def ready_piece(slot, piece, row=None):
            piece_arrived(slot, piece)
            whiten_lanes(slot, False, piece * quarter, quarter)
            if row is not None:
                rotate_chunk(row, slot, piece, 1)

        flow = Flow(False)
        start_own(flow)
        relay(END)
        ready(SIDE, 1)
        flow.task(0, SIDE)
        ready(MID)
        flow.task(0, MID)
        sends.append(push(cols.at[MID], cols.at[FAR], FAR, 9, near))
        ready(END, 2)
        flow.advance(0, 0)
        relay(END + 1)
        ready(MID + 1)
        flow.task(0, MID + 1)
        ready(END + 1, 2)
        flow.task(2, MID + 1)
        ready(SIDE + 1, 1)
        for row, slot in ((1, MID), (1, MID + 1), (0, SIDE + 1)):
            flow.task(row, slot, x_lag=6)
        flow.advance(0, 3)
        for ch in range(2):
            ready_piece(END_SIDE + ch, 0, 3)
        ready(FAR)
        for row in (2, 1, 0):
            flow.task(row, FAR, x_lag=6)
        for ch in range(2):
            ready_piece(END_SIDE + ch, 1, 3)
        for slot in (FAR, MID + 1):
            away[len(flow.done)] = guests[slot]
            flow.task(3, slot, x_lag=6)
        ready_piece(FAR + 1, 0)
        for row in (3, 2, 1, 0):
            flow.task(row, FAR + 1, 0, quarter, x_lag=6)
        for s in range(segs):
            for wave in range(2):
                segment_copy(raw_kept.at[1], s, wave, mid).wait_recv()
            whiten_lanes(FAR + 1, False, quarter, quarter, s)
            for row in (3, 2, 1, 0):
                if s == segs - 1:
                    flow.task(row, FAR + 1, quarter, quarter, x_lag=4, last=s)
                else:
                    begin(row, FAR + 1, quarter, quarter, s)
                    flow.advance(0, 5)
            flow.advance(1, 3) if s == segs - 1 else flow.advance(0, 4)
        expected = [(index, chunk) for index in (0, 1, 2, 3, 8, 9, 10)] + [(11, quarter), (12, quarter)]
        leave(flow, sends, expected)


def widen(steps, src, out, wide, out_sem):
    rows = src.shape[0] // steps
    ranges = [pl.ds(step * rows, rows) for step in range(steps)]
    stores = [pltpu.make_async_copy(wide.at[at], out.at[at], out_sem.at[i]) for i, at in enumerate(ranges)]
    for at, store in zip(ranges, stores):
        wide[at, :] = src[at, :].astype(jnp.float32)
        store.start()
    for store in stores:
        store.wait()


def fused_body(spectra, bin_index):
    parts, segs, bins, stations = spectra.shape
    blocks = lax.axis_size("sta")
    depth = parts * segs * bins
    chunk = stations // 2
    quarter = chunk // 2
    scale = 1.0 / math.sqrt(segs * lax.axis_size("seg") * bins)
    tasks = 24
    low = jnp.bfloat16
    out = pl.pallas_call(
        functools.partial(kernel, (segs, bins, chunk, scale)),
        out_shape=pltpu.VMEM((LAGS * quarter, blocks * stations), low),
        in_specs=[
            pl.BlockSpec(memory_space=pl.ANY),
            pl.BlockSpec(memory_space=pltpu.VMEM),
        ],
        out_specs=pl.BlockSpec(memory_space=pltpu.VMEM),
        scratch_shapes=[
            pltpu.VMEM((12, depth, chunk), low),
            pltpu.VMEM((2, depth, chunk), low),
            pltpu.VMEM((4, 2, LAGS * chunk, depth), low),
            pltpu.VMEM((tasks, 2, 2, LAGS * quarter, chunk), low),
            pltpu.VMEM((tasks, 2, LAGS * quarter, chunk), low),
            pltpu.VMEM((tasks, LAGS * quarter, chunk), low),
            pltpu.VMEM((bins, bins), low),
            pltpu.VMEM((bins, chunk), jnp.float32),
            pltpu.VMEM((4, 2, LAGS * chunk, quarter), jnp.float32),
            pltpu.VMEM((LAGS, bins), jnp.float32),
            pltpu.VMEM((LAGS, bins), jnp.float32),
            pltpu.SemaphoreType.DMA((2,)),
            pltpu.SemaphoreType.DMA((10 + 2 * segs, 2)),
            pltpu.SemaphoreType.DMA((15 + 2 * segs,)),
            pltpu.SemaphoreType.DMA((tasks,)),
            pltpu.SemaphoreType.DMA((tasks,)),
            pltpu.SemaphoreType.DMA((tasks,)),
            pltpu.SemaphoreType.DMA((tasks,)),
            pltpu.SemaphoreType.DMA((tasks,)),
            pltpu.SemaphoreType.DMA((14,)),
        ],
        compiler_params=pltpu.CompilerParams(
            collective_id=0, has_side_effects=True, vmem_limit_bytes=58 * 1024 * 1024
        ),
    )(spectra.reshape(depth, stations), bin_index.reshape(1, bins))
    return out.reshape(LAGS, quarter, blocks * stations).astype(jnp.float32)


def solution(mesh):
    placed = (P(None, "seg", None, "sta"), P())
    chosen = fused_body if (mesh.shape["sta"], mesh.shape["seg"]) == (8, 4) else general_body
    return jax.shard_map(
        chosen, mesh=mesh, in_specs=placed, out_specs=P(None, ("sta", "seg"), None), check_vma=False
    )
```

```python
import functools
import math

import jax
import jax.numpy as jnp
from jax import lax
from jax.experimental import pallas as pl
from jax.experimental.pallas import tpu as pltpu
from jax.sharding import PartitionSpec as P

NFFT = 8192
LAGS = 2
LAG_STEP = 37
HALF = 64
MESH = pl.DeviceIdType.MESH


def whiten(spectra):
    values = spectra.astype(jnp.float32)
    energy = values[0] * values[0] + values[1] * values[1]
    freq_bins = values.shape[2]
    bin_pos = jnp.arange(freq_bins, dtype=jnp.int32)
    window = (jnp.abs(bin_pos[:, None] - bin_pos[None, :]) <= HALF).astype(jnp.float32)
    bin_count = jnp.sum(window, axis=1)
    smoothed = (
        jnp.einsum("gf,sfc->sgc", window, energy, precision=lax.Precision.HIGHEST)
        / bin_count[None, :, None]
    )
    return (values / jnp.sqrt(smoothed + 1e-06)[None]).astype(jnp.bfloat16)


def phases(bin_index):
    lag_samples = (jnp.arange(LAGS, dtype=jnp.int32) + 1) * LAG_STEP
    phase_turn = lag_samples[:, None] * bin_index[None, :] % NFFT
    phase_angle = 2.0 * math.pi / NFFT * phase_turn.astype(jnp.float32)
    return (jnp.cos(phase_angle), jnp.sin(phase_angle))


def rotate(whitened, cosine, sine_part):
    real_part = whitened[0].astype(jnp.float32)[None]
    imag_part = whitened[1].astype(jnp.float32)[None]
    cos_part = cosine[:, None, :, None]
    sin_part = sine_part[:, None, :, None]
    rot_real = real_part * cos_part - imag_part * sin_part
    rot_imag = real_part * sin_part + imag_part * cos_part
    stacked = jnp.stack([rot_real, rot_imag], axis=1).astype(jnp.bfloat16)
    return stacked.reshape(cosine.shape[0], -1, whitened.shape[3])


def pair_block(rotated, columns, norm_scale):
    product = jnp.einsum("mki,kj->mij", rotated, columns, preferred_element_type=jnp.float32)
    return (product * norm_scale).astype(jnp.bfloat16)


def general_body(spectra, bin_index):
    whitened = whiten(spectra)
    cosine, sine_part = phases(bin_index)
    seg_local = whitened.shape[1]
    freq_bins = whitened.shape[2]
    norm_scale = 1.0 / math.sqrt(seg_local * lax.axis_size("seg") * freq_bins)
    rotated = rotate(whitened, cosine, sine_part)
    shard_cols = lax.all_gather(whitened, "sta", axis=3, tiled=True)
    columns = shard_cols.reshape(-1, shard_cols.shape[3])
    product = pair_block(rotated, columns, norm_scale)
    return lax.psum_scatter(product, "seg", scatter_dimension=1, tiled=True).astype(jnp.float32)


OWN, SIDE, END, END_SIDE, MID, FAR = 0, 2, 4, 6, 8, 10


def kernel(
    dims, src, bin_ref, out, cols, raw_kept, rows, part, from_core, from_x, window, inv_count, begun, cos_ref, sin_ref,
    load_sem, send_sem, recv_sem, core_send, core_recv, x_send, x_recv, out_send, out_recv,
):
    segs, bins, chunk, scale = dims
    depth = 2 * segs * bins
    half = segs * bins
    quarter = chunk // 2
    sta = lax.axis_index("sta")
    seg = lax.axis_index("seg")
    z, y = sta // 2, sta % 2
    x, core = seg // 2, seg % 2
    z_near = z + 1 - 2 * (z % 2)
    is_mid = ((z + 1) // 2) % 2
    side = z * 2 + (1 - y)
    near = z_near * 2 + y
    near_side = z_near * 2 + (1 - y)
    mid = (3 - z) * 2 + y
    far = ((z + 2) % 4) * 2 + y
    core_seg = x * 2 + (1 - core)
    x_seg = (1 - x) * 2 + core

    barrier = pltpu.get_barrier_semaphore()
    for partner in ((sta, core_seg), (sta, x_seg), (side, seg), (near, seg), (near_side, seg)):
        pl.semaphore_signal(barrier, inc=1, device_id=partner, device_id_type=MESH)

    @pl.when(is_mid == 1)
    def _():
        pl.semaphore_signal(barrier, inc=1, device_id=(mid, seg), device_id_type=MESH)

    loads = [
        pltpu.make_async_copy(
            src.at[:, pl.ds(ch * chunk, chunk)], cols.at[OWN + ch], load_sem.at[ch]
        )
        for ch in range(2)
    ]
    for load in loads:
        load.start()
    pl.semaphore_wait(barrier, 5 + is_mid)

    def remote(source, target, send, recv, to_sta, to_seg):
        return pltpu.make_async_remote_copy(
            src_ref=source, dst_ref=target, send_sem=send, recv_sem=recv,
            device_id=(to_sta, to_seg), device_id_type=MESH,
        )

    def own_chunk(ch):
        return src.at[:, pl.ds(ch * chunk, chunk)]

    def landing(slot, ends):
        kept = SIDE if ends else END
        return raw_kept.at[slot - kept] if kept <= slot < kept + 2 else cols.at[slot]

    def push(source, target, slot, to_sta):
        remote(source, target, send_sem, recv_sem.at[slot], to_sta, seg).start()

    second = {FAR + 1: 12, END_SIDE: 13, END_SIDE + 1: 14}

    def segment_copy(source, s, wave, to_sta):
        at = (pl.ds(wave * half + s * bins, bins), pl.ds(quarter, quarter))
        return remote(
            source.at[at], cols.at[FAR + 1].at[at],
            send_sem, recv_sem.at[15 + 2 * s + wave], to_sta, seg,
        )

    def push_pieces(source, slot, to_sta):
        for piece in range(2):
            lanes = pl.ds(piece * quarter, quarter)
            if slot == FAR + 1 and piece == 1:
                for s in range(segs):
                    for wave in range(2):
                        copy = segment_copy(source, s, wave, to_sta)
                        copy.start()
                continue
            copy = remote(
                source.at[:, lanes], cols.at[slot, :, lanes],
                send_sem, recv_sem.at[second[slot] if piece else slot], to_sta, seg,
            )
            copy.start()

    def piece_arrived(slot, piece):
        there = cols.at[slot, :, pl.ds(piece * quarter, quarter)]
        remote(
            there, there, send_sem, recv_sem.at[second[slot] if piece else slot], side, seg
        ).wait_recv()

    def arrived(slot, ends):
        there = landing(slot, ends)
        remote(there, there, send_sem, recv_sem.at[slot], side, seg).wait_recv()


    row_at = lax.broadcasted_iota(jnp.int32, (bins, bins), 0)
    col_at = lax.broadcasted_iota(jnp.int32, (bins, bins), 1)
    band = jnp.where(jnp.abs(row_at - col_at) <= HALF, 1.0, 0.0).astype(jnp.bfloat16)
    window[...] = band
    pos = lax.broadcasted_iota(jnp.int32, (bins, chunk), 0)
    count = jnp.minimum(pos, HALF) + jnp.minimum(bins - 1 - pos, HALF) + 1
    inv_count[...] = 1.0 / count.astype(jnp.float32)

    for lag in range(LAGS):
        turn = lax.rem((lag + 1) * LAG_STEP * bin_ref[...], NFFT)
        angle = 2.0 * math.pi / NFFT * turn.astype(jnp.float32)
        cos_ref[lag : lag + 1, :] = jnp.cos(angle)
        sin_ref[lag : lag + 1, :] = jnp.sin(angle)

    def rows_of(wave, s):
        start = wave * half + s * bins
        return pl.ds(start if isinstance(start, int) else pl.multiple_of(start, bins), bins)

    def whiten_lanes(slot, ends, first, width, only=None):
        raw = landing(slot, ends)
        lanes = pl.ds(first, width)

        def one(s, carry):
            at_re = rows_of(0, s)
            at_im = rows_of(1, s)
            real = raw[at_re, lanes].astype(jnp.float32)
            imag = raw[at_im, lanes].astype(jnp.float32)
            energy = real * real + imag * imag
            total = jnp.dot(window[...], energy.astype(jnp.bfloat16), preferred_element_type=jnp.float32)
            gain = lax.rsqrt(total * inv_count[:, :width] + 1e-06)
            real = raw[at_re, lanes].astype(jnp.float32)
            imag = raw[at_im, lanes].astype(jnp.float32)
            cols[slot, at_re, lanes] = (real * gain).astype(jnp.bfloat16)
            cols[slot, at_im, lanes] = (imag * gain).astype(jnp.bfloat16)
            return carry

        if only is None:
            lax.fori_loop(0, segs, one, 0)
        else:
            one(only, 0)

    def whiten_chunk(slot, ends):
        whiten_lanes(slot, ends, 0, chunk)

    def rotate_chunk(row, slot, first=0, pieces=2):
        xq = slot % 2

        def one(step, carry):
            parity, s = first + step // segs, step % segs
            lanes = pl.ds(pl.multiple_of(parity * quarter, quarter), quarter)
            at_re = pl.ds(pl.multiple_of(s * bins, bins), bins)
            at_im = pl.ds(pl.multiple_of(half + s * bins, bins), bins)
            real = cols[slot, at_re, lanes].T.astype(jnp.float32)
            imag = cols[slot, at_im, lanes].T.astype(jnp.float32)
            for lag in range(LAGS):
                cosine = cos_ref[lag : lag + 1, :]
                sine = sin_ref[lag : lag + 1, :]
                at = pl.ds(xq * LAGS * quarter + lag * quarter, quarter)
                rows[row, parity, at, at_re] = (real * cosine - imag * sine).astype(jnp.bfloat16)
                rows[row, parity, at, at_im] = (real * sine + imag * cosine).astype(jnp.bfloat16)
            return carry

        lax.fori_loop(0, pieces * segs, one, 0)

    def group(width):
        return 0 if width == chunk else 1

    def all_sent(sem, count, room, width):
        if count > 0:
            sent = room.at[pl.ds(0, count)]
            lanes = (slice(None),) * (len(room.shape) - 1) + (pl.ds(0, width),)
            sent = sent if width == chunk else sent.at[lanes]
            remote(sent, sent, sem, recv_sem.at[0], side, seg).wait_send()

    away = {}
    guests = {FAR: 14, MID + 1: 15}

    def away_copy(task):
        index, slot = task[0], task[2]
        return remote(
            part.at[index, 1], part.at[away[index], 1], out_send.at[2], out_recv.at[slot - 4], near_side, seg
        )

    def core_copy(task):
        index, width = task[0], task[4]
        return remote(
            part.at[index, 0, :, :, pl.ds(0, width)], from_core.at[index, :, :, pl.ds(0, width)],
            core_send.at[group(width)], core_recv.at[index], sta, core_seg,
        )

    def x_copy(task):
        index, width = task[0], task[4]
        return remote(
            part.at[index, 1, 1 - x, :, pl.ds(0, width)], from_x.at[index, :, pl.ds(0, width)],
            x_send.at[group(width)], x_recv.at[index], sta, x_seg,
        )

    def lanes_at(task, ends):
        index, row, slot, first, width = task
        if ends:
            station = {OWN: sta, SIDE: side, MID: near, FAR: far}[slot - slot % 2]
        else:
            station = {OWN: sta, SIDE: side, MID: mid, FAR: far}[slot - slot % 2]
        if ends and index in guests.values():
            station = (((z + 2) % 4) if slot == MID + 1 else 3 - z) * 2 + (1 - y)
        start = (station * 4 + (slot % 2) * 2 + first // quarter) * quarter
        return pl.ds(pl.multiple_of(start, quarter), width)

    def out_copy(task, ends):
        index, row, slot, first, width = task
        source = part.at[index, 1, x, :, pl.ds(0, width)]
        target = out.at[:, lanes_at(task, ends)]
        to_sta = {1: side, 2: near, 3: near_side}[row]
        if first > 0:
            arrival = 13 if row == 3 else 12
        elif row == 3:
            arrival = slot - 4
        elif row == 1 and ends:
            arrival = slot - MID
        else:
            arrival = slot
        return remote(source, target, out_send.at[group(width)], out_recv.at[arrival], to_sta, seg)

    def dot_segment(row, parity, slot, lanes, s):
        return sum(
            jnp.dot(
                rows[row, parity, :, rows_of(wave, s)], cols[slot, rows_of(wave, s), lanes],
                preferred_element_type=jnp.float32,
            )
            for wave in range(2)
        )

    def begin(row, slot, first, width, s):
        def one(h, carry):
            product = dot_segment(row, (core + 1 + h) % 2, slot, pl.ds(first, width), s)
            begun[row, h] = product if s == 0 else begun[row, h] + product
            return carry

        lax.fori_loop(0, 2, one, 0)

    def compute(task, last):
        index, row, slot, first, width = task
        lanes = pl.ds(first, width)

        def one(h, carry):
            parity = (core + 1 + h) % 2
            if last is None:
                product = jnp.dot(rows[row, parity], cols[slot, :, lanes], preferred_element_type=jnp.float32)
            else:
                product = dot_segment(row, parity, slot, lanes, last)
                if last > 0:
                    product = begun[row, h] + product
            product = (product * scale).astype(jnp.bfloat16)
            part[index, h, 0, :, :width] = product[: LAGS * quarter]
            part[index, h, 1, :, :width] = product[LAGS * quarter :]

            @pl.when(h == 0)
            def _():
                core_copy(task).start()

            return carry

        lax.fori_loop(0, 2, one, 0)

    def add_into(index, xq, other, width):
        def one(step, carry):
            at = pl.ds(pl.multiple_of(step * 64, 64), 64)
            mine = part[index, 1, xq, at, :width].astype(jnp.float32)
            part[index, 1, xq, at, :width] = (mine + other[at, :width].astype(jnp.float32)).astype(jnp.bfloat16)
            return carry

        lax.fori_loop(0, LAGS * quarter // 64, one, 0)

    def finish_core(task):
        index, width = task[0], task[4]
        core_copy(task).wait_recv()
        add_into(index, 1 - x, from_core.at[index, 1 - x], width)
        if index not in away:
            x_copy(task).start()
        add_into(index, x, from_core.at[index, x], width)
        if index in away:
            away_copy(task).start()

    def finish_x(task, ends):
        index, width = task[0], task[4]
        if index in away:
            return
        x_copy(task).wait_recv()
        if task[1] > 0:
            add_into(index, x, from_x.at[index], width)
            out_copy(task, ends).start()
            return
        lanes = lanes_at(task, ends)

        def one(step, carry):
            at = pl.ds(pl.multiple_of(step * 64, 64), 64)
            mine = part[index, 1, x, at, :width].astype(jnp.float32)
            out[at, lanes] = (mine + from_x[index, at, :width].astype(jnp.float32)).astype(jnp.bfloat16)
            return carry

        lax.fori_loop(0, LAGS * quarter // 64, one, 0)

    class Flow:
        def __init__(self, ends):
            self.ends = ends
            self.done = []
            self.guests = []
            self.at_core = 0
            self.at_x = 0

        def task(self, row, slot, first=0, width=chunk, core_lag=1, x_lag=3, last=None):
            self.done.append((len(self.done), row, slot, first, width))
            compute(self.done[-1], last)
            self.advance(core_lag, x_lag)

        def advance(self, core_lag, x_lag):
            while self.at_core < len(self.done) - core_lag:
                finish_core(self.done[self.at_core])
                self.at_core += 1
            while self.at_x < len(self.done) - x_lag:
                finish_x(self.done[self.at_x], self.ends)
                self.at_x += 1

        def drain(self):
            self.advance(0, 0)
            for width in (chunk, quarter):
                same = [task for task in self.done if task[4] == width]
                by_x = [task for task in same if task[0] not in away]
                moved = [task for task in by_x if task[1] > 0]
                guest_count = len(self.guests) if width == chunk else 0
                all_sent(core_send.at[group(width)], len(same), from_core, width)
                all_sent(x_send.at[group(width)], len(by_x) + guest_count, from_x, width)
                all_sent(out_send.at[group(width)], len(moved), from_x, width)
            all_sent(out_send.at[2], len([task for task in self.done if task[0] in away]), from_core, chunk)

    def incoming(index, width):
        target = out.at[:, pl.ds(0, width)]
        remote(target, target, out_send.at[0], out_recv.at[index], side, seg).wait_recv()

    def start_own(flow):
        for ch in range(2):
            loads[ch].wait()
            whiten_chunk(OWN + ch, flow.ends)
            rotate_chunk(0, OWN + ch)
        for ch in range(2):
            flow.task(0, OWN + ch)
        flow.advance(0, 0)

    def leave(flow, chunks_sent, expected):
        flow.drain()
        all_sent(send_sem, chunks_sent, cols, chunk)
        for index, width in expected:
            incoming(index, width)

    @pl.when(is_mid == 0)
    def _():
        for ch in range(2):
            push(own_chunk(ch), raw_kept.at[ch], END + ch, near)
            push(own_chunk(ch), raw_kept.at[ch], SIDE + ch, side)
        flow = Flow(True)
        start_own(flow)
        for ch in range(2):
            arrived(SIDE + ch, True)
            if ch == 0:
                push_pieces(raw_kept.at[0], END_SIDE, near)
            whiten_chunk(SIDE + ch, True)
            rotate_chunk(1, SIDE + ch)
            flow.task(0, SIDE + ch)
            arrived(MID + ch, True)
            whiten_chunk(MID + ch, True)
            rotate_chunk(2, MID + ch)
            flow.task(0, MID + ch)
            if ch == 0:
                flow.advance(0, 0)
        for row, slot in ((2, OWN), (2, OWN + 1), (2, SIDE), (2, SIDE + 1), (1, MID), (1, MID + 1)):
            flow.task(row, slot)
        arrived(FAR, True)
        flow.task(1, FAR)
        flow.task(0, FAR)
        flow.advance(0, 0)
        for slot in (FAR, MID + 1):
            index = guests[slot]
            there = part.at[index, 1]
            remote(there, there, send_sem, out_recv.at[slot - 4], near_side, seg).wait_recv()
            flow.guests.append((index, 0, slot, 0, chunk))
            x_copy(flow.guests[-1]).start()
        for task in flow.guests:
            finish_x(task, True)
        expected = [(index, chunk) for index in (0, 1, 2, 9, 10)]
        expected += [(7, quarter), (11, quarter), (12, quarter), (13, quarter)]
        leave(flow, 5, expected)

    @pl.when(is_mid == 1)
    def _():
        for ch in range(2):
            push(own_chunk(ch), cols.at[MID + ch], MID + ch, mid)
            push(own_chunk(ch), cols.at[SIDE + ch], SIDE + ch, side)
            push(own_chunk(ch), cols.at[MID + ch], MID + ch, near)

        def relay(slot):
            arrived(slot, False)
            if slot == END:
                push(raw_kept.at[0], cols.at[FAR], FAR, mid)
                return
            push_pieces(raw_kept.at[1], FAR + 1, mid)
            push_pieces(raw_kept.at[1], END_SIDE + 1, side)

        def ready(slot, row=None):
            if not END <= slot < END + 2:
                arrived(slot, False)
            whiten_chunk(slot, False)
            if row is not None:
                rotate_chunk(row, slot)

        def ready_piece(slot, piece, row=None):
            piece_arrived(slot, piece)
            whiten_lanes(slot, False, piece * quarter, quarter)
            if row is not None:
                rotate_chunk(row, slot, piece, 1)

        flow = Flow(False)
        start_own(flow)
        relay(END)
        ready(SIDE, 1)
        flow.task(0, SIDE)
        ready(MID)
        flow.task(0, MID)
        push(cols.at[MID], cols.at[FAR], FAR, near)
        ready(END, 2)
        flow.advance(0, 0)
        relay(END + 1)
        ready(MID + 1)
        flow.task(0, MID + 1)
        ready(END + 1, 2)
        flow.task(2, MID + 1)
        ready(SIDE + 1, 1)
        for row, slot in ((1, MID), (1, MID + 1), (0, SIDE + 1)):
            flow.task(row, slot, x_lag=6)
        flow.advance(0, 3)
        for ch in range(2):
            ready_piece(END_SIDE + ch, 0, 3)
        ready(FAR)
        for row in (2, 1, 0):
            flow.task(row, FAR, x_lag=6)
        for ch in range(2):
            ready_piece(END_SIDE + ch, 1, 3)
        for slot in (FAR, MID + 1):
            away[len(flow.done)] = guests[slot]
            flow.task(3, slot, x_lag=6)
        ready_piece(FAR + 1, 0)
        for row in (3, 2, 1, 0):
            flow.task(row, FAR + 1, 0, quarter, x_lag=6)
        for s in range(segs):
            for wave in range(2):
                segment_copy(raw_kept.at[1], s, wave, mid).wait_recv()
            whiten_lanes(FAR + 1, False, quarter, quarter, s)
            for row in (3, 2, 1, 0):
                if s == segs - 1:
                    flow.task(row, FAR + 1, quarter, quarter, x_lag=4, last=s)
                else:
                    begin(row, FAR + 1, quarter, quarter, s)
                    flow.advance(0, 5)
            flow.advance(1, 3) if s == segs - 1 else flow.advance(0, 4)
        expected = [(index, chunk) for index in (0, 1, 2, 3, 8, 9, 10)] + [(11, quarter), (12, quarter)]
        leave(flow, 10, expected)


def widen(steps, src, out, wide, out_sem):
    rows = src.shape[0] // steps
    ranges = [pl.ds(step * rows, rows) for step in range(steps)]
    stores = [pltpu.make_async_copy(wide.at[at], out.at[at], out_sem.at[i]) for i, at in enumerate(ranges)]
    for at, store in zip(ranges, stores):
        wide[at, :] = src[at, :].astype(jnp.float32)
        store.start()
    for store in stores:
        store.wait()


def fused_body(spectra, bin_index):
    parts, segs, bins, stations = spectra.shape
    blocks = lax.axis_size("sta")
    depth = parts * segs * bins
    chunk = stations // 2
    quarter = chunk // 2
    scale = 1.0 / math.sqrt(segs * lax.axis_size("seg") * bins)
    tasks = 24
    low = jnp.bfloat16
    out = pl.pallas_call(
        functools.partial(kernel, (segs, bins, chunk, scale)),
        out_shape=pltpu.VMEM((LAGS * quarter, blocks * stations), low),
        in_specs=[
            pl.BlockSpec(memory_space=pl.ANY),
            pl.BlockSpec(memory_space=pltpu.VMEM),
        ],
        out_specs=pl.BlockSpec(memory_space=pltpu.VMEM),
        scratch_shapes=[
            pltpu.VMEM((12, depth, chunk), low),
            pltpu.VMEM((2, depth, chunk), low),
            pltpu.VMEM((4, 2, LAGS * chunk, depth), low),
            pltpu.VMEM((tasks, 2, 2, LAGS * quarter, chunk), low),
            pltpu.VMEM((tasks, 2, LAGS * quarter, chunk), low),
            pltpu.VMEM((tasks, LAGS * quarter, chunk), low),
            pltpu.VMEM((bins, bins), low),
            pltpu.VMEM((bins, chunk), jnp.float32),
            pltpu.VMEM((4, 2, LAGS * chunk, quarter), jnp.float32),
            pltpu.VMEM((LAGS, bins), jnp.float32),
            pltpu.VMEM((LAGS, bins), jnp.float32),
            pltpu.SemaphoreType.DMA((2,)),
            pltpu.SemaphoreType.DMA,
            pltpu.SemaphoreType.DMA((15 + 2 * segs,)),
            pltpu.SemaphoreType.DMA((2,)),
            pltpu.SemaphoreType.DMA((tasks,)),
            pltpu.SemaphoreType.DMA((2,)),
            pltpu.SemaphoreType.DMA((tasks,)),
            pltpu.SemaphoreType.DMA((3,)),
            pltpu.SemaphoreType.DMA((14,)),
        ],
        compiler_params=pltpu.CompilerParams(
            collective_id=0, has_side_effects=True, vmem_limit_bytes=58 * 1024 * 1024
        ),
    )(spectra.reshape(depth, stations), bin_index.reshape(1, bins))
    return out.reshape(LAGS, quarter, blocks * stations).astype(jnp.float32)


def solution(mesh):
    placed = (P(None, "seg", None, "sta"), P())
    chosen = fused_body if (mesh.shape["sta"], mesh.shape["seg"]) == (8, 4) else general_body
    return jax.shard_map(
        chosen, mesh=mesh, in_specs=placed, out_specs=P(None, ("sta", "seg"), None), check_vma=False
    )
```

```python
import functools
import math

import jax
import jax.numpy as jnp
from jax import lax
from jax.experimental import pallas as pl
from jax.experimental.pallas import tpu as pltpu
from jax.sharding import PartitionSpec as P

NFFT = 8192
LAGS = 2
LAG_STEP = 37
HALF = 64
MESH = pl.DeviceIdType.MESH


def whiten(spectra):
    values = spectra.astype(jnp.float32)
    energy = values[0] * values[0] + values[1] * values[1]
    freq_bins = values.shape[2]
    bin_pos = jnp.arange(freq_bins, dtype=jnp.int32)
    window = (jnp.abs(bin_pos[:, None] - bin_pos[None, :]) <= HALF).astype(jnp.float32)
    bin_count = jnp.sum(window, axis=1)
    smoothed = (
        jnp.einsum("gf,sfc->sgc", window, energy, precision=lax.Precision.HIGHEST)
        / bin_count[None, :, None]
    )
    return (values / jnp.sqrt(smoothed + 1e-06)[None]).astype(jnp.bfloat16)


def phases(bin_index):
    lag_samples = (jnp.arange(LAGS, dtype=jnp.int32) + 1) * LAG_STEP
    phase_turn = lag_samples[:, None] * bin_index[None, :] % NFFT
    phase_angle = 2.0 * math.pi / NFFT * phase_turn.astype(jnp.float32)
    return (jnp.cos(phase_angle), jnp.sin(phase_angle))


def rotate(whitened, cosine, sine_part):
    real_part = whitened[0].astype(jnp.float32)[None]
    imag_part = whitened[1].astype(jnp.float32)[None]
    cos_part = cosine[:, None, :, None]
    sin_part = sine_part[:, None, :, None]
    rot_real = real_part * cos_part - imag_part * sin_part
    rot_imag = real_part * sin_part + imag_part * cos_part
    stacked = jnp.stack([rot_real, rot_imag], axis=1).astype(jnp.bfloat16)
    return stacked.reshape(cosine.shape[0], -1, whitened.shape[3])


def pair_block(rotated, columns, norm_scale):
    product = jnp.einsum("mki,kj->mij", rotated, columns, preferred_element_type=jnp.float32)
    return (product * norm_scale).astype(jnp.bfloat16)


def general_body(spectra, bin_index):
    whitened = whiten(spectra)
    cosine, sine_part = phases(bin_index)
    seg_local = whitened.shape[1]
    freq_bins = whitened.shape[2]
    norm_scale = 1.0 / math.sqrt(seg_local * lax.axis_size("seg") * freq_bins)
    rotated = rotate(whitened, cosine, sine_part)
    shard_cols = lax.all_gather(whitened, "sta", axis=3, tiled=True)
    columns = shard_cols.reshape(-1, shard_cols.shape[3])
    product = pair_block(rotated, columns, norm_scale)
    return lax.psum_scatter(product, "seg", scatter_dimension=1, tiled=True).astype(jnp.float32)


OWN, SIDE, END, END_SIDE, MID, FAR = 0, 2, 4, 6, 8, 10


def kernel(
    dims, src, bin_ref, out, cols, raw_kept, rows, part, from_core, from_x, window, inv_count, begun, cos_ref, sin_ref,
    load_sem, send_sem, recv_sem, core_send, core_recv, x_send, x_recv, out_send, out_recv,
):
    segs, bins, chunk, scale = dims
    depth = 2 * segs * bins
    half = segs * bins
    quarter = chunk // 2
    sta = lax.axis_index("sta")
    seg = lax.axis_index("seg")
    z, y = sta // 2, sta % 2
    x, core = seg // 2, seg % 2
    z_near = z + 1 - 2 * (z % 2)
    is_mid = ((z + 1) // 2) % 2
    side = z * 2 + (1 - y)
    near = z_near * 2 + y
    near_side = z_near * 2 + (1 - y)
    mid = (3 - z) * 2 + y
    far = ((z + 2) % 4) * 2 + y
    core_seg = x * 2 + (1 - core)
    x_seg = (1 - x) * 2 + core

    barrier = pltpu.get_barrier_semaphore()
    for partner in ((sta, core_seg), (sta, x_seg), (side, seg), (near, seg), (near_side, seg)):
        pl.semaphore_signal(barrier, inc=1, device_id=partner, device_id_type=MESH)

    @pl.when(is_mid == 1)
    def _():
        pl.semaphore_signal(barrier, inc=1, device_id=(mid, seg), device_id_type=MESH)

    loads = [
        pltpu.make_async_copy(
            src.at[:, pl.ds(ch * chunk, chunk)], cols.at[OWN + ch], load_sem.at[ch]
        )
        for ch in range(2)
    ]
    for load in loads:
        load.start()
    pl.semaphore_wait(barrier, 5 + is_mid)

    def remote(source, target, send, recv, to_sta, to_seg):
        return pltpu.make_async_remote_copy(
            src_ref=source, dst_ref=target, send_sem=send, recv_sem=recv,
            device_id=(to_sta, to_seg), device_id_type=MESH,
        )

    def own_chunk(ch):
        return src.at[:, pl.ds(ch * chunk, chunk)]

    def landing(slot, ends):
        kept = SIDE if ends else END
        return raw_kept.at[slot - kept] if kept <= slot < kept + 2 else cols.at[slot]

    def push(source, target, slot, to_sta):
        remote(source, target, send_sem, recv_sem.at[slot], to_sta, seg).start()

    second = {FAR + 1: 12, END_SIDE: 13, END_SIDE + 1: 14}

    def segment_copy(source, s, wave, to_sta):
        at = (pl.ds(wave * half + s * bins, bins), pl.ds(quarter, quarter))
        return remote(
            source.at[at], cols.at[FAR + 1].at[at],
            send_sem, recv_sem.at[15 + 2 * s + wave], to_sta, seg,
        )

    def push_pieces(source, slot, to_sta):
        for piece in range(2):
            lanes = pl.ds(piece * quarter, quarter)
            if slot == FAR + 1 and piece == 1:
                for s in range(segs):
                    for wave in range(2):
                        copy = segment_copy(source, s, wave, to_sta)
                        copy.start()
                continue
            copy = remote(
                source.at[:, lanes], cols.at[slot, :, lanes],
                send_sem, recv_sem.at[second[slot] if piece else slot], to_sta, seg,
            )
            copy.start()

    def piece_arrived(slot, piece):
        there = cols.at[slot, :, pl.ds(piece * quarter, quarter)]
        remote(
            there, there, send_sem, recv_sem.at[second[slot] if piece else slot], side, seg
        ).wait_recv()

    def arrived(slot, ends):
        there = landing(slot, ends)
        remote(there, there, send_sem, recv_sem.at[slot], side, seg).wait_recv()


    row_at = lax.broadcasted_iota(jnp.int32, (bins, bins), 0)
    col_at = lax.broadcasted_iota(jnp.int32, (bins, bins), 1)
    band = jnp.where(jnp.abs(row_at - col_at) <= HALF, 1.0, 0.0).astype(jnp.bfloat16)
    window[...] = band
    pos = lax.broadcasted_iota(jnp.int32, (bins, chunk), 0)
    count = jnp.minimum(pos, HALF) + jnp.minimum(bins - 1 - pos, HALF) + 1
    inv_count[...] = 1.0 / count.astype(jnp.float32)

    for lag in range(LAGS):
        turn = lax.rem((lag + 1) * LAG_STEP * bin_ref[...], NFFT)
        angle = 2.0 * math.pi / NFFT * turn.astype(jnp.float32)
        cos_ref[lag : lag + 1, :] = jnp.cos(angle)
        sin_ref[lag : lag + 1, :] = jnp.sin(angle)

    def rows_of(wave, s):
        start = wave * half + s * bins
        return pl.ds(start if isinstance(start, int) else pl.multiple_of(start, bins), bins)

    def whiten_lanes(slot, ends, first, width, only=None):
        raw = landing(slot, ends)
        lanes = pl.ds(first, width)

        def one(s, carry):
            at_re = rows_of(0, s)
            at_im = rows_of(1, s)
            real = raw[at_re, lanes].astype(jnp.float32)
            imag = raw[at_im, lanes].astype(jnp.float32)
            energy = real * real + imag * imag
            total = jnp.dot(window[...], energy.astype(jnp.bfloat16), preferred_element_type=jnp.float32)
            gain = lax.rsqrt(total * inv_count[:, :width] + 1e-06)
            real = raw[at_re, lanes].astype(jnp.float32)
            imag = raw[at_im, lanes].astype(jnp.float32)
            cols[slot, at_re, lanes] = (real * gain).astype(jnp.bfloat16)
            cols[slot, at_im, lanes] = (imag * gain).astype(jnp.bfloat16)
            return carry

        if only is None:
            lax.fori_loop(0, segs, one, 0)
        else:
            one(only, 0)

    def whiten_chunk(slot, ends):
        whiten_lanes(slot, ends, 0, chunk)

    def rotate_chunk(row, slot, first=0, pieces=2):
        xq = slot % 2

        def one(step, carry):
            parity, s = first + step // segs, step % segs
            lanes = pl.ds(pl.multiple_of(parity * quarter, quarter), quarter)
            at_re = pl.ds(pl.multiple_of(s * bins, bins), bins)
            at_im = pl.ds(pl.multiple_of(half + s * bins, bins), bins)
            real = cols[slot, at_re, lanes].T.astype(jnp.float32)
            imag = cols[slot, at_im, lanes].T.astype(jnp.float32)
            for lag in range(LAGS):
                cosine = cos_ref[lag : lag + 1, :]
                sine = sin_ref[lag : lag + 1, :]
                at = pl.ds(xq * LAGS * quarter + lag * quarter, quarter)
                rows[row, parity, at, at_re] = (real * cosine - imag * sine).astype(jnp.bfloat16)
                rows[row, parity, at, at_im] = (real * sine + imag * cosine).astype(jnp.bfloat16)
            return carry

        lax.fori_loop(0, pieces * segs, one, 0)

    def group(width):
        return 0 if width == chunk else 1

    def all_sent(sem, count, room, width):
        if count > 0:
            sent = room.at[pl.ds(0, count)]
            lanes = (slice(None),) * (len(room.shape) - 1) + (pl.ds(0, width),)
            sent = sent if width == chunk else sent.at[lanes]
            remote(sent, sent, sem, recv_sem.at[0], side, seg).wait_send()

    away = {}
    guests = {FAR: 14, MID + 1: 15}

    def away_copy(task):
        index, slot = task[0], task[2]
        return remote(
            part.at[index, 1], part.at[away[index], 1], out_send.at[2], out_recv.at[guests[slot] - 13], near_side, seg
        )

    def core_copy(task):
        index, width = task[0], task[4]
        return remote(
            part.at[index, 0, :, :, pl.ds(0, width)], from_core.at[index, :, :, pl.ds(0, width)],
            core_send.at[group(width)], core_recv.at[index], sta, core_seg,
        )

    def x_copy(task):
        index, width = task[0], task[4]
        return remote(
            part.at[index, 1, 1 - x, :, pl.ds(0, width)], from_x.at[index, :, pl.ds(0, width)],
            x_send.at[group(width)], x_recv.at[index], sta, x_seg,
        )

    def lanes_at(task, ends):
        index, row, slot, first, width = task
        if ends:
            station = {OWN: sta, SIDE: side, MID: near, FAR: far}[slot - slot % 2]
        else:
            station = {OWN: sta, SIDE: side, MID: mid, FAR: far}[slot - slot % 2]
        if ends and index in guests.values():
            station = (((z + 2) % 4) if slot == MID + 1 else 3 - z) * 2 + (1 - y)
        start = (station * 4 + (slot % 2) * 2 + first // quarter) * quarter
        return pl.ds(pl.multiple_of(start, quarter), width)

    def out_copy(task, ends):
        index, row, slot, first, width = task
        source = part.at[index, 1, x, :, pl.ds(0, width)]
        target = out.at[:, lanes_at(task, ends)]
        to_sta = {1: side, 2: near, 3: near_side}[row]
        return remote(source, target, out_send.at[group(width)], out_recv.at[0], to_sta, seg)

    def dot_segment(row, parity, slot, lanes, s):
        return sum(
            jnp.dot(
                rows[row, parity, :, rows_of(wave, s)], cols[slot, rows_of(wave, s), lanes],
                preferred_element_type=jnp.float32,
            )
            for wave in range(2)
        )

    def begin(row, slot, first, width, s):
        def one(h, carry):
            product = dot_segment(row, (core + 1 + h) % 2, slot, pl.ds(first, width), s)
            begun[row, h] = product if s == 0 else begun[row, h] + product
            return carry

        lax.fori_loop(0, 2, one, 0)

    def compute(task, last):
        index, row, slot, first, width = task
        lanes = pl.ds(first, width)

        def one(h, carry):
            parity = (core + 1 + h) % 2
            if last is None:
                product = jnp.dot(rows[row, parity], cols[slot, :, lanes], preferred_element_type=jnp.float32)
            else:
                product = dot_segment(row, parity, slot, lanes, last)
                if last > 0:
                    product = begun[row, h] + product
            product = (product * scale).astype(jnp.bfloat16)
            part[index, h, 0, :, :width] = product[: LAGS * quarter]
            part[index, h, 1, :, :width] = product[LAGS * quarter :]

            @pl.when(h == 0)
            def _():
                core_copy(task).start()

            return carry

        lax.fori_loop(0, 2, one, 0)

    def add_into(index, xq, other, width):
        def one(step, carry):
            at = pl.ds(pl.multiple_of(step * 64, 64), 64)
            mine = part[index, 1, xq, at, :width].astype(jnp.float32)
            part[index, 1, xq, at, :width] = (mine + other[at, :width].astype(jnp.float32)).astype(jnp.bfloat16)
            return carry

        lax.fori_loop(0, LAGS * quarter // 64, one, 0)

    def finish_core(task):
        index, width = task[0], task[4]
        core_copy(task).wait_recv()
        add_into(index, 1 - x, from_core.at[index, 1 - x], width)
        if index not in away:
            x_copy(task).start()
        add_into(index, x, from_core.at[index, x], width)
        if index in away:
            away_copy(task).start()

    def finish_x(task, ends):
        index, width = task[0], task[4]
        if index in away:
            return
        x_copy(task).wait_recv()
        if task[1] > 0:
            add_into(index, x, from_x.at[index], width)
            out_copy(task, ends).start()
            return
        lanes = lanes_at(task, ends)

        def one(step, carry):
            at = pl.ds(pl.multiple_of(step * 64, 64), 64)
            mine = part[index, 1, x, at, :width].astype(jnp.float32)
            out[at, lanes] = (mine + from_x[index, at, :width].astype(jnp.float32)).astype(jnp.bfloat16)
            return carry

        lax.fori_loop(0, LAGS * quarter // 64, one, 0)

    class Flow:
        def __init__(self, ends):
            self.ends = ends
            self.done = []
            self.guests = []
            self.at_core = 0
            self.at_x = 0

        def task(self, row, slot, first=0, width=chunk, core_lag=1, x_lag=3, last=None):
            self.done.append((len(self.done), row, slot, first, width))
            compute(self.done[-1], last)
            self.advance(core_lag, x_lag)

        def advance(self, core_lag, x_lag):
            while self.at_core < len(self.done) - core_lag:
                finish_core(self.done[self.at_core])
                self.at_core += 1
            while self.at_x < len(self.done) - x_lag:
                finish_x(self.done[self.at_x], self.ends)
                self.at_x += 1

        def drain(self):
            self.advance(0, 0)
            for width in (chunk, quarter):
                same = [task for task in self.done if task[4] == width]
                by_x = [task for task in same if task[0] not in away]
                moved = [task for task in by_x if task[1] > 0]
                guest_count = len(self.guests) if width == chunk else 0
                all_sent(core_send.at[group(width)], len(same), from_core, width)
                all_sent(x_send.at[group(width)], len(by_x) + guest_count, from_x, width)
                all_sent(out_send.at[group(width)], len(moved), from_x, width)
            all_sent(out_send.at[2], len([task for task in self.done if task[0] in away]), from_core, chunk)

    def start_own(flow):
        for ch in range(2):
            loads[ch].wait()
            whiten_chunk(OWN + ch, flow.ends)
            rotate_chunk(0, OWN + ch)
        for ch in range(2):
            flow.task(0, OWN + ch)
        flow.advance(0, 0)

    def leave(flow, chunks_sent, tiles):
        flow.drain()
        all_sent(send_sem, chunks_sent, cols, chunk)
        room = from_x.at[pl.ds(0, tiles)]
        remote(room, room, send_sem, out_recv.at[0], side, seg).wait_recv()

    @pl.when(is_mid == 0)
    def _():
        for ch in range(2):
            push(own_chunk(ch), raw_kept.at[ch], END + ch, near)
            push(own_chunk(ch), raw_kept.at[ch], SIDE + ch, side)
        flow = Flow(True)
        start_own(flow)
        for ch in range(2):
            arrived(SIDE + ch, True)
            if ch == 0:
                push_pieces(raw_kept.at[0], END_SIDE, near)
            whiten_chunk(SIDE + ch, True)
            rotate_chunk(1, SIDE + ch)
            flow.task(0, SIDE + ch)
            arrived(MID + ch, True)
            whiten_chunk(MID + ch, True)
            rotate_chunk(2, MID + ch)
            flow.task(0, MID + ch)
            if ch == 0:
                flow.advance(0, 0)
        for row, slot in ((2, OWN), (2, OWN + 1), (2, SIDE), (2, SIDE + 1), (1, MID), (1, MID + 1)):
            flow.task(row, slot)
        arrived(FAR, True)
        flow.task(1, FAR)
        flow.task(0, FAR)
        flow.advance(0, 0)
        for slot in (FAR, MID + 1):
            index = guests[slot]
            there = part.at[index, 1]
            remote(there, there, send_sem, out_recv.at[guests[slot] - 13], near_side, seg).wait_recv()
            flow.guests.append((index, 0, slot, 0, chunk))
            x_copy(flow.guests[-1]).start()
        for task in flow.guests:
            finish_x(task, True)
        leave(flow, 5, 7)

    @pl.when(is_mid == 1)
    def _():
        for ch in range(2):
            push(own_chunk(ch), cols.at[MID + ch], MID + ch, mid)
            push(own_chunk(ch), cols.at[SIDE + ch], SIDE + ch, side)
            push(own_chunk(ch), cols.at[MID + ch], MID + ch, near)

        def relay(slot):
            arrived(slot, False)
            if slot == END:
                push(raw_kept.at[0], cols.at[FAR], FAR, mid)
                return
            push_pieces(raw_kept.at[1], FAR + 1, mid)
            push_pieces(raw_kept.at[1], END_SIDE + 1, side)

        def ready(slot, row=None):
            if not END <= slot < END + 2:
                arrived(slot, False)
            whiten_chunk(slot, False)
            if row is not None:
                rotate_chunk(row, slot)

        def ready_piece(slot, piece, row=None):
            piece_arrived(slot, piece)
            whiten_lanes(slot, False, piece * quarter, quarter)
            if row is not None:
                rotate_chunk(row, slot, piece, 1)

        flow = Flow(False)
        start_own(flow)
        relay(END)
        ready(SIDE, 1)
        flow.task(0, SIDE)
        ready(MID)
        flow.task(0, MID)
        push(cols.at[MID], cols.at[FAR], FAR, near)
        ready(END, 2)
        flow.advance(0, 0)
        relay(END + 1)
        ready(MID + 1)
        flow.task(0, MID + 1)
        ready(END + 1, 2)
        flow.task(2, MID + 1)
        ready(SIDE + 1, 1)
        for row, slot in ((1, MID), (1, MID + 1), (0, SIDE + 1)):
            flow.task(row, slot, x_lag=6)
        flow.advance(0, 3)
        for ch in range(2):
            ready_piece(END_SIDE + ch, 0, 3)
        ready(FAR)
        for row in (2, 1, 0):
            flow.task(row, FAR, x_lag=6)
        for ch in range(2):
            ready_piece(END_SIDE + ch, 1, 3)
        for slot in (FAR, MID + 1):
            away[len(flow.done)] = guests[slot]
            flow.task(3, slot, x_lag=6)
        ready_piece(FAR + 1, 0)
        for row in (3, 2, 1, 0):
            flow.task(row, FAR + 1, 0, quarter, x_lag=6)
        for s in range(segs):
            for wave in range(2):
                segment_copy(raw_kept.at[1], s, wave, mid).wait_recv()
            whiten_lanes(FAR + 1, False, quarter, quarter, s)
            for row in (3, 2, 1, 0):
                if s == segs - 1:
                    flow.task(row, FAR + 1, quarter, quarter, x_lag=4, last=s)
                else:
                    begin(row, FAR + 1, quarter, quarter, s)
                    flow.advance(0, 5)
            flow.advance(1, 3) if s == segs - 1 else flow.advance(0, 4)
        leave(flow, 10, 8)


def widen(steps, src, out, wide, out_sem):
    rows = src.shape[0] // steps
    ranges = [pl.ds(step * rows, rows) for step in range(steps)]
    stores = [pltpu.make_async_copy(wide.at[at], out.at[at], out_sem.at[i]) for i, at in enumerate(ranges)]
    for at, store in zip(ranges, stores):
        wide[at, :] = src[at, :].astype(jnp.float32)
        store.start()
    for store in stores:
        store.wait()


def fused_body(spectra, bin_index):
    parts, segs, bins, stations = spectra.shape
    blocks = lax.axis_size("sta")
    depth = parts * segs * bins
    chunk = stations // 2
    quarter = chunk // 2
    scale = 1.0 / math.sqrt(segs * lax.axis_size("seg") * bins)
    tasks = 24
    low = jnp.bfloat16
    out = pl.pallas_call(
        functools.partial(kernel, (segs, bins, chunk, scale)),
        out_shape=pltpu.VMEM((LAGS * quarter, blocks * stations), low),
        in_specs=[
            pl.BlockSpec(memory_space=pl.ANY),
            pl.BlockSpec(memory_space=pltpu.VMEM),
        ],
        out_specs=pl.BlockSpec(memory_space=pltpu.VMEM),
        scratch_shapes=[
            pltpu.VMEM((12, depth, chunk), low),
            pltpu.VMEM((2, depth, chunk), low),
            pltpu.VMEM((4, 2, LAGS * chunk, depth), low),
            pltpu.VMEM((tasks, 2, 2, LAGS * quarter, chunk), low),
            pltpu.VMEM((tasks, 2, LAGS * quarter, chunk), low),
            pltpu.VMEM((tasks, LAGS * quarter, chunk), low),
            pltpu.VMEM((bins, bins), low),
            pltpu.VMEM((bins, chunk), jnp.float32),
            pltpu.VMEM((4, 2, LAGS * chunk, quarter), jnp.float32),
            pltpu.VMEM((LAGS, bins), jnp.float32),
            pltpu.VMEM((LAGS, bins), jnp.float32),
            pltpu.SemaphoreType.DMA((2,)),
            pltpu.SemaphoreType.DMA,
            pltpu.SemaphoreType.DMA((15 + 2 * segs,)),
            pltpu.SemaphoreType.DMA((2,)),
            pltpu.SemaphoreType.DMA((tasks,)),
            pltpu.SemaphoreType.DMA((2,)),
            pltpu.SemaphoreType.DMA((tasks,)),
            pltpu.SemaphoreType.DMA((3,)),
            pltpu.SemaphoreType.DMA((3,)),
        ],
        compiler_params=pltpu.CompilerParams(
            collective_id=0, has_side_effects=True, vmem_limit_bytes=58 * 1024 * 1024
        ),
    )(spectra.reshape(depth, stations), bin_index.reshape(1, bins))
    return out.reshape(LAGS, quarter, blocks * stations).astype(jnp.float32)


def solution(mesh):
    placed = (P(None, "seg", None, "sta"), P())
    chosen = fused_body if (mesh.shape["sta"], mesh.shape["seg"]) == (8, 4) else general_body
    return jax.shard_map(
        chosen, mesh=mesh, in_specs=placed, out_specs=P(None, ("sta", "seg"), None), check_vma=False
    )
```

```python
import functools
import math

import jax
import jax.numpy as jnp
from jax import lax
from jax.experimental import pallas as pl
from jax.experimental.pallas import tpu as pltpu
from jax.sharding import PartitionSpec as P

NFFT = 8192
LAGS = 2
LAG_STEP = 37
HALF = 64
MESH = pl.DeviceIdType.MESH


def whiten(spectra):
    values = spectra.astype(jnp.float32)
    energy = values[0] * values[0] + values[1] * values[1]
    freq_bins = values.shape[2]
    bin_pos = jnp.arange(freq_bins, dtype=jnp.int32)
    window = (jnp.abs(bin_pos[:, None] - bin_pos[None, :]) <= HALF).astype(jnp.float32)
    bin_count = jnp.sum(window, axis=1)
    smoothed = (
        jnp.einsum("gf,sfc->sgc", window, energy, precision=lax.Precision.HIGHEST)
        / bin_count[None, :, None]
    )
    return (values / jnp.sqrt(smoothed + 1e-06)[None]).astype(jnp.bfloat16)


def phases(bin_index):
    lag_samples = (jnp.arange(LAGS, dtype=jnp.int32) + 1) * LAG_STEP
    phase_turn = lag_samples[:, None] * bin_index[None, :] % NFFT
    phase_angle = 2.0 * math.pi / NFFT * phase_turn.astype(jnp.float32)
    return (jnp.cos(phase_angle), jnp.sin(phase_angle))


def rotate(whitened, cosine, sine_part):
    real_part = whitened[0].astype(jnp.float32)[None]
    imag_part = whitened[1].astype(jnp.float32)[None]
    cos_part = cosine[:, None, :, None]
    sin_part = sine_part[:, None, :, None]
    rot_real = real_part * cos_part - imag_part * sin_part
    rot_imag = real_part * sin_part + imag_part * cos_part
    stacked = jnp.stack([rot_real, rot_imag], axis=1).astype(jnp.bfloat16)
    return stacked.reshape(cosine.shape[0], -1, whitened.shape[3])


def pair_block(rotated, columns, norm_scale):
    product = jnp.einsum("mki,kj->mij", rotated, columns, preferred_element_type=jnp.float32)
    return (product * norm_scale).astype(jnp.bfloat16)


def general_body(spectra, bin_index):
    whitened = whiten(spectra)
    cosine, sine_part = phases(bin_index)
    seg_local = whitened.shape[1]
    freq_bins = whitened.shape[2]
    norm_scale = 1.0 / math.sqrt(seg_local * lax.axis_size("seg") * freq_bins)
    rotated = rotate(whitened, cosine, sine_part)
    shard_cols = lax.all_gather(whitened, "sta", axis=3, tiled=True)
    columns = shard_cols.reshape(-1, shard_cols.shape[3])
    product = pair_block(rotated, columns, norm_scale)
    return lax.psum_scatter(product, "seg", scatter_dimension=1, tiled=True).astype(jnp.float32)


OWN, SIDE, END, END_SIDE, MID, FAR = 0, 2, 4, 6, 8, 10


def kernel(
    dims, src, bin_ref, out, cols, raw_kept, rows, part, from_core, from_x, window, inv_count, begun, cos_ref, sin_ref,
    load_sem, send_sem, recv_sem, core_send, core_recv, x_send, x_recv, out_send, out_recv,
):
    segs, bins, chunk, scale = dims
    depth = 2 * segs * bins
    half = segs * bins
    quarter = chunk // 2
    sta = lax.axis_index("sta")
    seg = lax.axis_index("seg")
    z, y = sta // 2, sta % 2
    x, core = seg // 2, seg % 2
    z_near = z + 1 - 2 * (z % 2)
    is_mid = ((z + 1) // 2) % 2
    side = z * 2 + (1 - y)
    near = z_near * 2 + y
    near_side = z_near * 2 + (1 - y)
    mid = (3 - z) * 2 + y
    far = ((z + 2) % 4) * 2 + y
    core_seg = x * 2 + (1 - core)
    x_seg = (1 - x) * 2 + core

    barrier = pltpu.get_barrier_semaphore()
    for partner in ((sta, core_seg), (sta, x_seg), (side, seg), (near, seg), (near_side, seg)):
        pl.semaphore_signal(barrier, inc=1, device_id=partner, device_id_type=MESH)

    @pl.when(is_mid == 1)
    def _():
        pl.semaphore_signal(barrier, inc=1, device_id=(mid, seg), device_id_type=MESH)

    loads = [
        pltpu.make_async_copy(
            src.at[:, pl.ds(ch * chunk, chunk)], cols.at[OWN + ch], load_sem.at[ch]
        )
        for ch in range(2)
    ]
    for load in loads:
        load.start()
    pl.semaphore_wait(barrier, 5 + is_mid)

    def remote(source, target, send, recv, to_sta, to_seg):
        return pltpu.make_async_remote_copy(
            src_ref=source, dst_ref=target, send_sem=send, recv_sem=recv,
            device_id=(to_sta, to_seg), device_id_type=MESH,
        )

    def own_chunk(ch):
        return src.at[:, pl.ds(ch * chunk, chunk)]

    def landing(slot, ends):
        kept = SIDE if ends else END
        return raw_kept.at[slot - kept] if kept <= slot < kept + 2 else cols.at[slot]

    def push(source, target, slot, to_sta):
        remote(source, target, send_sem, recv_sem.at[slot], to_sta, seg).start()

    second = {FAR + 1: 12, END_SIDE: 13, END_SIDE + 1: 14}

    def segment_copy(source, s, wave, to_sta):
        at = (pl.ds(wave * half + s * bins, bins), pl.ds(quarter, quarter))
        return remote(
            source.at[at], cols.at[FAR + 1].at[at],
            send_sem, recv_sem.at[15 + 2 * s + wave], to_sta, seg,
        )

    def push_pieces(source, slot, to_sta):
        for piece in range(2):
            lanes = pl.ds(piece * quarter, quarter)
            if slot == FAR + 1 and piece == 1:
                for s in range(segs):
                    for wave in range(2):
                        copy = segment_copy(source, s, wave, to_sta)
                        copy.start()
                continue
            copy = remote(
                source.at[:, lanes], cols.at[slot, :, lanes],
                send_sem, recv_sem.at[second[slot] if piece else slot], to_sta, seg,
            )
            copy.start()

    def piece_arrived(slot, piece):
        there = cols.at[slot, :, pl.ds(piece * quarter, quarter)]
        remote(
            there, there, send_sem, recv_sem.at[second[slot] if piece else slot], side, seg
        ).wait_recv()

    def arrived(slot, ends):
        there = landing(slot, ends)
        remote(there, there, send_sem, recv_sem.at[slot], side, seg).wait_recv()


    row_at = lax.broadcasted_iota(jnp.int32, (bins, bins), 0)
    col_at = lax.broadcasted_iota(jnp.int32, (bins, bins), 1)
    band = jnp.where(jnp.abs(row_at - col_at) <= HALF, 1.0, 0.0).astype(jnp.bfloat16)
    window[...] = band
    pos = lax.broadcasted_iota(jnp.int32, (bins, chunk), 0)
    count = jnp.minimum(pos, HALF) + jnp.minimum(bins - 1 - pos, HALF) + 1
    inv_count[...] = 1.0 / count.astype(jnp.float32)

    for lag in range(LAGS):
        turn = lax.rem((lag + 1) * LAG_STEP * bin_ref[...], NFFT)
        angle = 2.0 * math.pi / NFFT * turn.astype(jnp.float32)
        cos_ref[lag : lag + 1, :] = jnp.cos(angle)
        sin_ref[lag : lag + 1, :] = jnp.sin(angle)

    def rows_of(wave, s):
        start = wave * half + s * bins
        return pl.ds(start if isinstance(start, int) else pl.multiple_of(start, bins), bins)

    def whiten_lanes(slot, ends, first, width, only=None):
        raw = landing(slot, ends)
        lanes = pl.ds(first, width)

        def one(s, carry):
            at_re = rows_of(0, s)
            at_im = rows_of(1, s)
            real = raw[at_re, lanes].astype(jnp.float32)
            imag = raw[at_im, lanes].astype(jnp.float32)
            energy = real * real + imag * imag
            total = jnp.dot(window[...], energy.astype(jnp.bfloat16), preferred_element_type=jnp.float32)
            gain = lax.rsqrt(total * inv_count[:, :width] + 1e-06)
            real = raw[at_re, lanes].astype(jnp.float32)
            imag = raw[at_im, lanes].astype(jnp.float32)
            cols[slot, at_re, lanes] = (real * gain).astype(jnp.bfloat16)
            cols[slot, at_im, lanes] = (imag * gain).astype(jnp.bfloat16)
            return carry

        if only is None:
            lax.fori_loop(0, segs, one, 0)
        else:
            one(only, 0)

    def whiten_chunk(slot, ends):
        whiten_lanes(slot, ends, 0, chunk)

    def rotate_chunk(row, slot, first=0, pieces=2):
        xq = slot % 2

        def one(step, carry):
            parity, s = first + step // segs, step % segs
            lanes = pl.ds(pl.multiple_of(parity * quarter, quarter), quarter)
            at_re = pl.ds(pl.multiple_of(s * bins, bins), bins)
            at_im = pl.ds(pl.multiple_of(half + s * bins, bins), bins)
            real = cols[slot, at_re, lanes].T.astype(jnp.float32)
            imag = cols[slot, at_im, lanes].T.astype(jnp.float32)
            for lag in range(LAGS):
                cosine = cos_ref[lag : lag + 1, :]
                sine = sin_ref[lag : lag + 1, :]
                at = pl.ds(xq * LAGS * quarter + lag * quarter, quarter)
                rows[row, parity, at, at_re] = (real * cosine - imag * sine).astype(jnp.bfloat16)
                rows[row, parity, at, at_im] = (real * sine + imag * cosine).astype(jnp.bfloat16)
            return carry

        lax.fori_loop(0, pieces * segs, one, 0)

    def group(width):
        return 0 if width == chunk else 1

    def all_sent(sem, count, room, width):
        if count > 0:
            sent = room.at[pl.ds(0, count)]
            lanes = (slice(None),) * (len(room.shape) - 1) + (pl.ds(0, width),)
            sent = sent if width == chunk else sent.at[lanes]
            remote(sent, sent, sem, recv_sem.at[0], side, seg).wait_send()

    away = {}
    guests = {FAR: 14, MID + 1: 15}

    def away_copy(task):
        index, slot = task[0], task[2]
        return remote(
            part.at[index, 1], part.at[away[index], 1], out_send.at[2], out_recv.at[slot - 4], near_side, seg
        )

    def core_copy(task):
        index, width = task[0], task[4]
        return remote(
            part.at[index, 0, :, :, pl.ds(0, width)], from_core.at[index, :, :, pl.ds(0, width)],
            core_send.at[group(width)], core_recv.at[index], sta, core_seg,
        )

    def x_copy(task):
        index, width = task[0], task[4]
        return remote(
            part.at[index, 1, 1 - x, :, pl.ds(0, width)], from_x.at[index, :, pl.ds(0, width)],
            x_send.at[group(width)], x_recv.at[index], sta, x_seg,
        )

    def lanes_at(task, ends):
        index, row, slot, first, width = task
        if ends:
            station = {OWN: sta, SIDE: side, MID: near, FAR: far}[slot - slot % 2]
        else:
            station = {OWN: sta, SIDE: side, MID: mid, FAR: far}[slot - slot % 2]
        if ends and index in guests.values():
            station = (((z + 2) % 4) if slot == MID + 1 else 3 - z) * 2 + (1 - y)
        start = (station * 4 + (slot % 2) * 2 + first // quarter) * quarter
        return pl.ds(pl.multiple_of(start, quarter), width)

    def out_copy(task, ends):
        index, row, slot, first, width = task
        source = part.at[index, 1, x, :, pl.ds(0, width)]
        target = out.at[:, lanes_at(task, ends)]
        to_sta = {1: side, 2: near, 3: near_side}[row]
        if first > 0:
            arrival = 13 if row == 3 else 12
        elif row == 3:
            arrival = slot - 4
        elif row == 1 and ends:
            arrival = slot - MID
        else:
            arrival = slot
        return remote(source, target, out_send.at[group(width)], out_recv.at[arrival], to_sta, seg)

    def dot_segment(row, parity, slot, lanes, s):
        return sum(
            jnp.dot(
                rows[row, parity, :, rows_of(wave, s)], cols[slot, rows_of(wave, s), lanes],
                preferred_element_type=jnp.float32,
            )
            for wave in range(2)
        )

    def begin(row, slot, first, width, s):
        def one(h, carry):
            product = dot_segment(row, (core + 1 + h) % 2, slot, pl.ds(first, width), s)
            begun[row, h] = product if s == 0 else begun[row, h] + product
            return carry

        lax.fori_loop(0, 2, one, 0)

    def compute(task, last):
        index, row, slot, first, width = task
        lanes = pl.ds(first, width)

        def one(h, carry):
            parity = (core + 1 + h) % 2
            if last is None:
                product = jnp.dot(rows[row, parity], cols[slot, :, lanes], preferred_element_type=jnp.float32)
            else:
                product = dot_segment(row, parity, slot, lanes, last)
                if last > 0:
                    product = begun[row, h] + product
            product = (product * scale).astype(jnp.bfloat16)
            part[index, h, 0, :, :width] = product[: LAGS * quarter]
            part[index, h, 1, :, :width] = product[LAGS * quarter :]

            @pl.when(h == 0)
            def _():
                core_copy(task).start()

            return carry

        lax.fori_loop(0, 2, one, 0)

    def add_into(index, xq, other, width):
        def one(step, carry):
            at = pl.ds(pl.multiple_of(step * 64, 64), 64)
            mine = part[index, 1, xq, at, :width].astype(jnp.float32)
            part[index, 1, xq, at, :width] = (mine + other[at, :width].astype(jnp.float32)).astype(jnp.bfloat16)
            return carry

        lax.fori_loop(0, LAGS * quarter // 64, one, 0)

    def finish_core(task):
        index, width = task[0], task[4]
        core_copy(task).wait_recv()
        add_into(index, 1 - x, from_core.at[index, 1 - x], width)
        if index not in away:
            x_copy(task).start()
        add_into(index, x, from_core.at[index, x], width)
        if index in away:
            away_copy(task).start()

    def finish_x(task, ends):
        index, width = task[0], task[4]
        if index in away:
            return
        x_copy(task).wait_recv()
        if task[1] > 0:
            add_into(index, x, from_x.at[index], width)
            out_copy(task, ends).start()
            return
        lanes = lanes_at(task, ends)

        def one(step, carry):
            at = pl.ds(pl.multiple_of(step * 64, 64), 64)
            mine = part[index, 1, x, at, :width].astype(jnp.float32)
            out[at, lanes] = (mine + from_x[index, at, :width].astype(jnp.float32)).astype(jnp.bfloat16)
            return carry

        lax.fori_loop(0, LAGS * quarter // 64, one, 0)

    class Flow:
        def __init__(self, ends):
            self.ends = ends
            self.done = []
            self.guests = []
            self.at_core = 0
            self.at_x = 0

        def task(self, row, slot, first=0, width=chunk, core_lag=1, x_lag=3, last=None):
            self.done.append((len(self.done), row, slot, first, width))
            compute(self.done[-1], last)
            self.advance(core_lag, x_lag)

        def advance(self, core_lag, x_lag):
            while self.at_core < len(self.done) - core_lag:
                finish_core(self.done[self.at_core])
                self.at_core += 1
            while self.at_x < len(self.done) - x_lag:
                finish_x(self.done[self.at_x], self.ends)
                self.at_x += 1

        def drain(self):
            self.advance(0, 0)
            for width in (chunk, quarter):
                same = [task for task in self.done if task[4] == width]
                by_x = [task for task in same if task[0] not in away]
                moved = [task for task in by_x if task[1] > 0]
                guest_count = len(self.guests) if width == chunk else 0
                all_sent(core_send.at[group(width)], len(same), from_core, width)
                all_sent(x_send.at[group(width)], len(by_x) + guest_count, from_x, width)
                all_sent(out_send.at[group(width)], len(moved), from_x, width)
            all_sent(out_send.at[2], len([task for task in self.done if task[0] in away]), from_core, chunk)

    def incoming(index, width):
        target = out.at[:, pl.ds(0, width)]
        remote(target, target, out_send.at[0], out_recv.at[index], side, seg).wait_recv()

    def start_own(flow):
        for ch in range(2):
            loads[ch].wait()
            whiten_chunk(OWN + ch, flow.ends)
            rotate_chunk(0, OWN + ch)
        for ch in range(2):
            flow.task(0, OWN + ch)
        flow.advance(0, 0)

    def leave(flow, chunks_sent, expected):
        flow.drain()
        all_sent(send_sem, chunks_sent, cols, chunk)
        for index, width in expected:
            incoming(index, width)

    @pl.when(is_mid == 0)
    def _():
        for ch in range(2):
            push(own_chunk(ch), raw_kept.at[ch], END + ch, near)
            push(own_chunk(ch), raw_kept.at[ch], SIDE + ch, side)
        flow = Flow(True)
        start_own(flow)
        for ch in range(2):
            arrived(SIDE + ch, True)
            if ch == 0:
                push_pieces(raw_kept.at[0], END_SIDE, near)
            whiten_chunk(SIDE + ch, True)
            rotate_chunk(1, SIDE + ch)
            flow.task(0, SIDE + ch)
            arrived(MID + ch, True)
            whiten_chunk(MID + ch, True)
            rotate_chunk(2, MID + ch)
            flow.task(0, MID + ch)
            if ch == 0:
                flow.advance(0, 0)
        for row, slot in ((2, OWN), (2, OWN + 1), (2, SIDE), (2, SIDE + 1), (1, MID), (1, MID + 1)):
            flow.task(row, slot)
        arrived(FAR, True)
        flow.task(1, FAR)
        flow.task(0, FAR)
        flow.advance(0, 0)
        for slot in (FAR, MID + 1):
            index = guests[slot]
            there = part.at[index, 1]
            remote(there, there, send_sem, out_recv.at[slot - 4], near_side, seg).wait_recv()
            flow.guests.append((index, 0, slot, 0, chunk))
            x_copy(flow.guests[-1]).start()
        for task in flow.guests:
            finish_x(task, True)
        expected = [(index, chunk) for index in (0, 1, 2, 9, 10)]
        expected += [(7, quarter), (11, quarter), (12, quarter), (13, quarter)]
        leave(flow, 5, expected)

    @pl.when(is_mid == 1)
    def _():
        for ch in range(2):
            push(own_chunk(ch), cols.at[MID + ch], MID + ch, mid)
            push(own_chunk(ch), cols.at[SIDE + ch], SIDE + ch, side)
            push(own_chunk(ch), cols.at[MID + ch], MID + ch, near)

        def relay(slot):
            arrived(slot, False)
            if slot == END:
                push(raw_kept.at[0], cols.at[FAR], FAR, mid)
                return
            push_pieces(raw_kept.at[1], FAR + 1, mid)
            push_pieces(raw_kept.at[1], END_SIDE + 1, side)

        def ready(slot, row=None):
            if not END <= slot < END + 2:
                arrived(slot, False)
            whiten_chunk(slot, False)
            if row is not None:
                rotate_chunk(row, slot)

        def ready_piece(slot, piece, row=None):
            piece_arrived(slot, piece)
            whiten_lanes(slot, False, piece * quarter, quarter)
            if row is not None:
                rotate_chunk(row, slot, piece, 1)

        flow = Flow(False)
        start_own(flow)
        relay(END)
        ready(SIDE, 1)
        flow.task(0, SIDE)
        ready(MID)
        flow.task(0, MID)
        push(cols.at[MID], cols.at[FAR], FAR, near)
        ready(END, 2)
        flow.advance(0, 0)
        relay(END + 1)
        ready(MID + 1)
        flow.task(0, MID + 1)
        ready(END + 1, 2)
        flow.task(2, MID + 1)
        ready(SIDE + 1, 1)
        for row, slot in ((1, MID), (1, MID + 1), (0, SIDE + 1)):
            flow.task(row, slot, x_lag=6)
        flow.advance(0, 3)
        for piece in range(2):
            for ch in range(2):
                ready_piece(END_SIDE + ch, piece, 3)
        ready(FAR)
        for row in (2, 1, 0):
            flow.task(row, FAR, x_lag=6)
        for slot in (FAR, MID + 1):
            away[len(flow.done)] = guests[slot]
            flow.task(3, slot, x_lag=6)
        ready_piece(FAR + 1, 0)
        for row in (3, 2, 1, 0):
            flow.task(row, FAR + 1, 0, quarter, x_lag=6)
        for s in range(segs):
            for wave in range(2):
                segment_copy(raw_kept.at[1], s, wave, mid).wait_recv()
            whiten_lanes(FAR + 1, False, quarter, quarter, s)
            for row in (3, 2, 1, 0):
                if s == segs - 1:
                    flow.task(row, FAR + 1, quarter, quarter, x_lag=4, last=s)
                else:
                    begin(row, FAR + 1, quarter, quarter, s)
                    flow.advance(0, 5)
            flow.advance(1, 3) if s == segs - 1 else flow.advance(0, 4)
        expected = [(index, chunk) for index in (0, 1, 2, 3, 8, 9, 10)] + [(11, quarter), (12, quarter)]
        leave(flow, 10, expected)


def widen(steps, src, out, wide, out_sem):
    rows = src.shape[0] // steps
    ranges = [pl.ds(step * rows, rows) for step in range(steps)]
    stores = [pltpu.make_async_copy(wide.at[at], out.at[at], out_sem.at[i]) for i, at in enumerate(ranges)]
    for at, store in zip(ranges, stores):
        wide[at, :] = src[at, :].astype(jnp.float32)
        store.start()
    for store in stores:
        store.wait()


def fused_body(spectra, bin_index):
    parts, segs, bins, stations = spectra.shape
    blocks = lax.axis_size("sta")
    depth = parts * segs * bins
    chunk = stations // 2
    quarter = chunk // 2
    scale = 1.0 / math.sqrt(segs * lax.axis_size("seg") * bins)
    tasks = 24
    low = jnp.bfloat16
    out = pl.pallas_call(
        functools.partial(kernel, (segs, bins, chunk, scale)),
        out_shape=pltpu.VMEM((LAGS * quarter, blocks * stations), low),
        in_specs=[
            pl.BlockSpec(memory_space=pl.ANY),
            pl.BlockSpec(memory_space=pltpu.VMEM),
        ],
        out_specs=pl.BlockSpec(memory_space=pltpu.VMEM),
        scratch_shapes=[
            pltpu.VMEM((12, depth, chunk), low),
            pltpu.VMEM((2, depth, chunk), low),
            pltpu.VMEM((4, 2, LAGS * chunk, depth), low),
            pltpu.VMEM((tasks, 2, 2, LAGS * quarter, chunk), low),
            pltpu.VMEM((tasks, 2, LAGS * quarter, chunk), low),
            pltpu.VMEM((tasks, LAGS * quarter, chunk), low),
            pltpu.VMEM((bins, bins), low),
            pltpu.VMEM((bins, chunk), jnp.float32),
            pltpu.VMEM((4, 2, LAGS * chunk, quarter), jnp.float32),
            pltpu.VMEM((LAGS, bins), jnp.float32),
            pltpu.VMEM((LAGS, bins), jnp.float32),
            pltpu.SemaphoreType.DMA((2,)),
            pltpu.SemaphoreType.DMA,
            pltpu.SemaphoreType.DMA((15 + 2 * segs,)),
            pltpu.SemaphoreType.DMA((2,)),
            pltpu.SemaphoreType.DMA((tasks,)),
            pltpu.SemaphoreType.DMA((2,)),
            pltpu.SemaphoreType.DMA((tasks,)),
            pltpu.SemaphoreType.DMA((3,)),
            pltpu.SemaphoreType.DMA((14,)),
        ],
        compiler_params=pltpu.CompilerParams(
            collective_id=0, has_side_effects=True, vmem_limit_bytes=58 * 1024 * 1024
        ),
    )(spectra.reshape(depth, stations), bin_index.reshape(1, bins))
    return out.reshape(LAGS, quarter, blocks * stations).astype(jnp.float32)


def solution(mesh):
    placed = (P(None, "seg", None, "sta"), P())
    chosen = fused_body if (mesh.shape["sta"], mesh.shape["seg"]) == (8, 4) else general_body
    return jax.shard_map(
        chosen, mesh=mesh, in_specs=placed, out_specs=P(None, ("sta", "seg"), None), check_vma=False
    )
```
